32 devices in a mesh: dp: 8 (over z, core), tp: 4 (over y, x).
Axes of the slice: x: 2, y: 2, z: 4, core: 2. Of those that a mesh axis runs over, the one named last changes fastest.
Arguments:
- hidden_states: bfloat16 [2048, 3584], P('dp'), may hold values from -21 to 21
- resp_lengths: int32 [4], replicated, may hold values from 1 to 1280, 2048 in all
- w_query: bfloat16 [3584, 512], P('dp', 'tp'), may hold values from -0.25 to 0.25
- w_keyval: bfloat16 [3584, 1024], P('dp', 'tp'), may hold values from -0.09375 to 0.09375
- w_out: bfloat16 [512, 3584], P('tp', 'dp'), may hold values from -0.25 to 0.25
Outputs:
- attended: bfloat16 [2048, 3584], P('dp', 'tp')
The draws below stay inside these ranges and needn't reach their ends.
Inputs may be any that keep to these rules, and one draw needn't show every extreme that they name: `resp_lengths`: the 4 lengths sum to 2048; the longest is exactly 1280.
All inputs are finite; a program needn't handle non-finite values.
Results may differ from the reference program's by a relative error of at most 0.015.
The reference program's roundings to bfloat16 on the way count: a program that leaves them out, or rounds other values in their place, can miss the bound.
Values may be sent and summed in bfloat16 or wider, within the bound.
A program may use at most 64 MiB of HBM per device.

```python
import math
import jax
import jax.numpy as jnp
import numpy as np
from jax import lax

D = 3584
HD = 128
KV = 4
TOK_DEV = 256
HEADS = 4
TOKENS = 2048
LMAX = 1280
NRESP = 4
N_TP = 4


def draw_hidden_states(key, part):
    first_key = jax.random.fold_in(jax.random.fold_in(key, 11), 0)
    values = jnp.clip(jax.random.normal(first_key, (TOKENS, D), jnp.float32), -6.0, 6.0)
    return values.astype(jnp.bfloat16)


def level_of(stream_key, extent, shards, low, high):
    factor_of = 1.0
    for dim, parts in shards:
        draws = jax.random.uniform(jax.random.fold_in(jax.random.fold_in(stream_key, 6), dim), (parts,), jnp.float32, low / len(shards), high / len(shards))
        factor_of = factor_of * jnp.repeat(jnp.exp(draws), extent[dim] // parts).reshape((-1,) + (1,) * (len(extent) - 1 - dim))
    return factor_of


def length_profile(amount, total, reach, slope):
    portions = [(1 << 20) // math.isqrt(grade ** slope) + 1 for grade in range(2, amount + 1)]
    surplus, holding = total - reach - (amount - 1), [1] * (amount - 1)
    while surplus > 0:
        free = [i for i in range(amount - 1) if holding[i] < reach]
        whole, budget = sum([portions[i] for i in free]), surplus
        for i in free:
            extra = min(reach - holding[i], max(1, budget * portions[i] // whole), surplus)
            holding[i] = holding[i] + extra
            surplus = surplus - extra
    return np.array([reach] + holding)


def uneven_parts(own_key, amount, total, limit, skew):
    if amount == 2:
        one = jax.random.randint(own_key, (), max(1, total - limit), min(limit, total - 1) + 1)
        return jnp.stack([one, total - one])
    tallies = jnp.asarray(length_profile(amount, total, limit, skew), jnp.int32)
    couples = (amount - 1) // 2
    donor, sink = tallies[1:1 + 2 * couples:2], tallies[2:2 + 2 * couples:2]
    room = jnp.minimum(donor - 1, limit - sink)
    moved = jax.random.randint(jax.random.fold_in(own_key, 1), (couples,), 0, 1 << 20) % (room + 1)
    tallies = tallies.at[1:1 + 2 * couples:2].set(donor - moved).at[2:2 + 2 * couples:2].set(sink + moved)
    return tallies[jax.random.permutation(jax.random.fold_in(own_key, 2), amount)]


def centred(own_key, shape, width, reach, pieces=(), kind=jnp.bfloat16):
    result = width * jax.random.normal(own_key, shape, jnp.float32)
    if pieces:
        result = result * level_of(own_key, shape, pieces, -0.22, 0.18)
    return jnp.clip(result, -reach, reach).astype(kind)


def setup_inputs(seed: int = 0) -> dict:
    key_list = jax.random.split(jax.random.key(seed), 6)
    hidden_states = draw_hidden_states(jax.random.fold_in(key_list[5], 71), 0)
    resp_lengths = uneven_parts(key_list[1], NRESP, TOKENS, LMAX, 2).astype(jnp.int32)
    w_query = centred(key_list[2], (D, HEADS * HD), (D // 6) ** -0.5, 0.25, ((0, 8), (1, 4)))
    w_keyval = centred(key_list[3], (D, 2 * KV * HD), D ** -0.5, 0.09375, ((0, 8), (1, 4)))
    w_out = centred(key_list[4], (HEADS * HD, D), (HEADS * HD) ** -0.5, 0.25, ((0, 4), (1, 8)))
    return dict(hidden_states=hidden_states, resp_lengths=resp_lengths, w_query=w_query, w_keyval=w_keyval, w_out=w_out)


def reference(hidden_states, resp_lengths, w_query, w_keyval, w_out):
    total_tokens = hidden_states.shape[0]
    head_scale = HD ** -0.5
    query = (jnp.dot(hidden_states, w_query, preferred_element_type=jnp.float32) * head_scale).astype(jnp.bfloat16)
    keyval = jnp.dot(hidden_states, w_keyval, preferred_element_type=jnp.float32).astype(jnp.bfloat16)
    resp_ends = jnp.cumsum(resp_lengths, dtype=jnp.int32)
    position = jnp.arange(total_tokens, dtype=jnp.int32)
    segment = jnp.sum((position[:, None] >= resp_ends[None, :]).astype(jnp.int32), axis=1, dtype=jnp.int32)
    window = min(total_tokens, TOK_DEV + LMAX)
    blocks = total_tokens // TOK_DEV
    per_group = HEADS // KV

    def one_head(head):
        kv_head = (head // per_group).astype(jnp.int32)
        key_head = lax.dynamic_slice_in_dim(keyval, kv_head * HD, HD, 1)
        value_head = lax.dynamic_slice_in_dim(keyval, (KV + kv_head) * HD, HD, 1)
        query_head = lax.dynamic_slice_in_dim(query, (head * HD).astype(jnp.int32), HD, 1)

        def one_block(block):
            begin = (block * TOK_DEV).astype(jnp.int32)
            key_begin = jnp.clip(begin + TOK_DEV - window, 0, total_tokens - window).astype(jnp.int32)
            query_rows = lax.dynamic_slice_in_dim(query_head, begin, TOK_DEV, 0)
            key_rows = lax.dynamic_slice_in_dim(key_head, key_begin, window, 0)
            value_rows = lax.dynamic_slice_in_dim(value_head, key_begin, window, 0)
            query_pos = begin + jnp.arange(TOK_DEV, dtype=jnp.int32)
            key_pos = key_begin + jnp.arange(window, dtype=jnp.int32)
            query_seg = lax.dynamic_slice_in_dim(segment, begin, TOK_DEV, 0)
            key_seg = lax.dynamic_slice_in_dim(segment, key_begin, window, 0)
            scores = jnp.dot(query_rows, key_rows.T, preferred_element_type=jnp.float32)
            allowed = (query_seg[:, None] == key_seg[None, :]) & (key_pos[None, :] <= query_pos[:, None])
            largest = jnp.max(jnp.where(allowed, scores, jnp.float32(-1e30)), axis=1)
            expw = jnp.where(allowed, jnp.exp(scores - largest[:, None]), jnp.float32(0.0))
            denom = jnp.sum(expw, axis=1)
            numer = jnp.dot(expw.astype(jnp.bfloat16), value_rows, preferred_element_type=jnp.float32)
            return (numer / denom[:, None]).astype(jnp.bfloat16)

        return lax.map(one_block, jnp.arange(blocks, dtype=jnp.int32)).reshape(total_tokens, HD)

    heads_all = lax.map(one_head, jnp.arange(HEADS, dtype=jnp.int32))
    heads_out = jnp.transpose(heads_all, (1, 0, 2)).reshape(total_tokens, HEADS * HD)
    group_width = (HEADS // N_TP) * HD
    summed = jnp.zeros((total_tokens, w_out.shape[1]), jnp.float32)
    for group in range(N_TP):
        partial_sum = jnp.dot(heads_out[:, group * group_width:(group + 1) * group_width],
                              w_out[group * group_width:(group + 1) * group_width],
                              preferred_element_type=jnp.float32).astype(jnp.bfloat16)
        partial_sum = lax.optimization_barrier(partial_sum)
        summed = summed + partial_sum.astype(jnp.float32)
    return summed.astype(jnp.bfloat16)
```

```python
import functools

import jax
import jax.numpy as jnp
from jax import lax
from jax.experimental import pallas as pl
from jax.experimental.pallas import tpu as pltpu
from jax.sharding import PartitionSpec as P

HD = 128


def segment_of(position, resp_ends):
    return jnp.sum(
        (position[:, None] >= resp_ends[None, :]).astype(jnp.int32), axis=1, dtype=jnp.int32
    )


def body(hidden_states, resp_lengths, w_query, w_keyval, w_out):
    token_rows = hidden_states.shape[0]
    head_scale = HD ** (-0.5)
    pieces = (
        lax.all_gather(w_query, "dp", axis=0, tiled=True),
        lax.all_gather(w_keyval, "dp", axis=0, tiled=True),
    )
    query_sum = jnp.dot(hidden_states, pieces[0], preferred_element_type=jnp.float32)
    keyval_sum = jnp.dot(hidden_states, pieces[1], preferred_element_type=jnp.float32)
    query = (query_sum * head_scale).astype(jnp.bfloat16)
    keyval = lax.all_gather(keyval_sum.astype(jnp.bfloat16), "tp", axis=1, tiled=True)
    kv_count = keyval.shape[1] // (2 * HD)
    per_group = lax.axis_size("tp") // kv_count
    kv_head = lax.axis_index("tp") // per_group
    key_head = lax.dynamic_slice_in_dim(keyval, kv_head * HD, HD, 1)
    value_head = lax.dynamic_slice_in_dim(keyval, (kv_count + kv_head) * HD, HD, 1)
    head_pair = jnp.concatenate([key_head, value_head], axis=1)
    resp_ends = jnp.cumsum(resp_lengths, dtype=jnp.int32)
    own_begin = lax.axis_index("dp") * token_rows
    query_pos = own_begin + jnp.arange(token_rows, dtype=jnp.int32)
    query_seg = segment_of(query_pos, resp_ends)
    pieces = lax.all_gather(head_pair, "dp", axis=0, tiled=True)
    largest = jnp.full((token_rows,), -1e30, jnp.float32)
    height = pieces.shape[0]
    key_pos = jnp.arange(height, dtype=jnp.int32)
    key_seg = segment_of(key_pos, resp_ends)
    scores = jnp.dot(query, pieces[:, :HD].T, preferred_element_type=jnp.float32)
    allowed = (
        (query_seg[:, None] == key_seg[None, :])
        & (key_pos[None, :] <= query_pos[:, None])
        & (key_pos[None, :] >= 0)
    )
    newest = jnp.maximum(largest, jnp.max(jnp.where(allowed, scores, jnp.float32(-1e30)), axis=1))
    expw = jnp.where(allowed, jnp.exp(scores - newest[:, None]), jnp.float32(0.0))
    denom = jnp.sum(expw, axis=1)
    numer = jnp.dot(expw.astype(jnp.bfloat16), pieces[:, HD:], preferred_element_type=jnp.float32)
    heads_out = (numer / denom[:, None]).astype(jnp.bfloat16)
    terms = jnp.dot(
        heads_out,
        lax.all_gather(w_out, "dp", axis=1, tiled=True),
        preferred_element_type=jnp.float32,
    )
    summed = lax.psum_scatter(terms.astype(jnp.bfloat16), "tp", scatter_dimension=1, tiled=True)
    return summed


MESH = pl.DeviceIdType.MESH
KA, KB, WQ = range(3)
UP, DOWN, SIDE = range(3)
NEG = -1e30


def fused_kernel(
    nz, nt, lens_ref, hid_hbm, wq_hbm, wkv_hbm, wo_hbm, out_ref,
    hid, w, woc, wof, kvloc, kvb, acc, qb, part, lse, pin, lin, hloc, hcat,
    loc_sem, ss, rs, prs, kv_ss, kv_rs, kp_ss, kp_rs, wi_ss, wi_rs, wp_ss, wp_rs,
    pt_ss, pt_rs, h_ss, h_rs,
):
    dp = lax.axis_index("dp")
    t = lax.axis_index("tp")
    plane_of, c = dp // 2, dp % 2
    rows = hid.shape[0]
    shard = wq_hbm.shape[0]
    nout = wo_hbm.shape[0]
    own = pl.ds(pl.multiple_of(dp * shard, 64), shard)

    loads = [
        pltpu.make_async_copy(wkv_hbm.at[:, pl.ds(0, HD)], w.at[KA, own], loc_sem.at[KA]),
        pltpu.make_async_copy(wkv_hbm.at[:, pl.ds(HD, HD)], w.at[KB, own], loc_sem.at[KB]),
        pltpu.make_async_copy(wq_hbm, w.at[WQ, own], loc_sem.at[WQ]),
        pltpu.make_async_copy(hid_hbm, hid, loc_sem.at[3]),
        pltpu.make_async_copy(wo_hbm, woc, loc_sem.at[4]),
    ]
    for load in loads:
        load.start()

    barrier = pltpu.get_barrier_semaphore()
    partner = {"dp": dp + 1 - 2 * c, "tp": t}
    above, below = {"dp": dp + 2, "tp": t}, {"dp": dp - 2, "tp": t}
    has_up, has_down = plane_of < nz - 1, plane_of > 0
    pl.semaphore_signal(barrier, 1, device_id=partner, device_id_type=MESH)

    @pl.when(has_up)
    def _():
        pl.semaphore_signal(barrier, 1, device_id=above, device_id_type=MESH)

    @pl.when(has_down)
    def _():
        pl.semaphore_signal(barrier, 1, device_id=below, device_id_type=MESH)

    for k in range(1, nt):
        pl.semaphore_signal(
            barrier, 1, device_id={"dp": dp, "tp": (t + k) % nt}, device_id_type=MESH
        )
    pl.semaphore_wait(barrier, nt + has_up.astype(jnp.int32) + has_down.astype(jnp.int32))

    def chunk(item, zz, cc):
        return w.at[item, pl.ds(pl.multiple_of((2 * zz + cc) * shard, 64), shard)]

    def remote(src, dst, send, recv, to):
        return pltpu.make_async_remote_copy(
            src, dst, send, recv, device_id=to, device_id_type=MESH
        )

    def chain(item, zz, way):
        ref = chunk(item, zz, c)
        recv = prs.at[item, zz] if way == SIDE else rs.at[item, zz]
        return remote(ref, ref, ss.at[item, zz, way], recv, (above, below, partner)[way])

    def device(zz, tt):
        return {"dp": 2 * zz + c, "tp": tt}

    half_rows = pl.ds(pl.multiple_of(c * rows, 128), rows)
    other_rows = pl.ds(pl.multiple_of((1 - c) * rows, 128), rows)

    def kv_copy(z, b, zz):
        role = t // (nt // 2)
        return remote(
            kvloc.at[b], kvb.at[role, z, half_rows], kv_ss.at[b, zz], kv_rs.at[role, z],
            device(zz, 2 * (t % (nt // 2)) + b),
        )

    def kv_pass(z, role):
        ref = kvb.at[role, z, half_rows]
        return remote(ref, ref, kp_ss.at[role, z], kp_rs.at[role, z], partner)

    def kv_passed(z, role):
        ref = kvb.at[role, z, other_rows]
        return remote(ref, ref, kp_ss.at[role, z], kp_rs.at[role, z], partner)

    def wo_block(g, cc):
        return wof.at[
            pl.ds(pl.multiple_of(cc * nout, 64), nout), pl.ds(pl.multiple_of(g * HD, HD), HD)
        ]

    def wo_copy(z, zz):
        return remote(woc, wo_block(t, c), wi_ss.at[zz], wi_rs.at[t], device(zz, z))

    def wo_pass(g, cc):
        ref = wo_block(g, cc)
        return remote(ref, ref, wp_ss.at[g], wp_rs.at[g], partner)

    def head_cols(g):
        return hcat.at[:, pl.ds(pl.multiple_of(g * HD, HD), HD)]

    def head_copy(k):
        return remote(
            hloc, head_cols(t), h_ss.at[k], h_rs.at[t], {"dp": dp, "tp": (t + k) % nt}
        )

    ends = []
    end = jnp.int32(0)
    for r in range(lens_ref.shape[0]):
        end = end + lens_ref[r]
        ends.append(end)

    def plane(z):
        sent = []
        seen = set()
        top, bottom = z == nz - 1, z == 0
        kv_to = [zz for zz in (nz - 2, nz - 3, 0) if zz >= z] if not top else [z]
        span = 2 * shard

        def go(copy):
            copy.start()
            sent.append(copy)

        def own_send(item, way):
            go(chain(item, z, way))

        def event(item, zz, *ways):
            ref = chunk(item, zz, c)
            remote(ref, ref, ss.at[item, zz, UP], rs.at[item, zz], partner).wait_recv()
            for way in ways + (SIDE,):
                go(chain(item, zz, way))

        def dot(item, zz):
            ref = chunk(item, zz, 1 - c)
            remote(ref, ref, ss.at[item, zz, SIDE], prs.at[item, zz], partner).wait_recv()
            part_sum = jnp.dot(
                hid[:, zz * span:(zz + 1) * span], w[item, zz * span:(zz + 1) * span, :],
                preferred_element_type=jnp.float32,
            )
            if item in seen:
                acc[item] += part_sum
            else:
                seen.add(item)
                acc[item] = part_sum

        def finish_kv(b):
            kvloc[b] = acc[b].astype(jnp.bfloat16)
            role = t // (nt // 2)
            for zz in kv_to:
                if zz != z:
                    go(kv_copy(z, b, zz))
            mine = 2 * (t % (nt // 2)) + b == t

            @pl.when(jnp.logical_not(mine))
            def _():
                kv_copy(z, b, z).start()

            @pl.when(mine)
            def _():
                kvb[role, z, half_rows, :] = kvloc[b]

        def end_kv():
            for b in range(2):
                @pl.when(2 * (t % (nt // 2)) + b != t)
                def _():
                    kv_copy(z, b, z).wait_send()

        def take_kv(zs):
            for role in range(2):
                arrived = remote(
                    kvloc.at[0], kvb.at[role, zs, half_rows], kv_ss.at[0, zs],
                    kv_rs.at[role, zs], partner,
                )
                if zs == z:
                    @pl.when(t // 2 + role * (nt // 2) != t)
                    def _():
                        arrived.wait_recv()
                else:
                    arrived.wait_recv()
                go(kv_pass(zs, role))

        def need_kv(zs):
            for role in range(2):
                kv_passed(zs, role).wait_recv()

        def finish_q():
            qb[0] = (acc[WQ] * (HD ** -0.5)).astype(jnp.bfloat16)

        def attend(state, qi, zs):
            qpos = (dp + 2 * qi) * rows + lax.broadcasted_iota(jnp.int32, (rows, 1), 0)
            first = jnp.zeros((rows, 1), jnp.int32)
            for e in ends:
                first = jnp.where(qpos >= e, e, first)
            s = lax.dot_general(
                qb[qi], kvb[0, zs], (((1,), (1,)), ((), ())), preferred_element_type=jnp.float32
            )
            kpos = zs * 2 * rows + lax.broadcasted_iota(jnp.int32, s.shape, 1)
            s = jnp.where((kpos >= first) & (kpos <= qpos), s, jnp.float32(NEG))
            peak = jnp.max(s, axis=1, keepdims=True)
            if state is not None:
                peak = jnp.maximum(state[0], peak)
            p = jnp.exp(s - peak)
            total = jnp.sum(p, axis=1, keepdims=True)
            value = jnp.dot(
                p.astype(jnp.bfloat16), kvb[1, zs], preferred_element_type=jnp.float32
            )
            if state is not None:
                fade = jnp.exp(state[0] - peak)
                total = total + state[1] * fade
                value = value + state[2] * fade
            return peak, total, value

        def wo_near():
            loads[4].wait()

            @pl.when(t != z)
            def _():
                wo_copy(z, z).start()

            @pl.when(t == z)
            def _():
                wo_block(t, c)[...] = woc[...]

        def wo_far(zz):
            go(wo_copy(z, zz))

        def query_copy():
            return remote(qb.at[0], qb.at[1], pt_ss.at[0], pt_rs.at[0], below)

        def part_copies(to):
            return (
                remote(part, pin, pt_ss.at[1], pt_rs.at[1], to),
                remote(lse, lin, pt_ss.at[2], pt_rs.at[2], to),
            )

        for item in (WQ, KA, KB):
            loads[item].wait()
            if not top and (bottom or item != KB):
                own_send(item, UP)
            if top or (not bottom and item != WQ):
                own_send(item, DOWN)
            own_send(item, SIDE)
        wo_near()
        loads[3].wait()

        waiting = [(WQ, z), (KA, z), (KB, z)]

        def step(item, zz, *ways, keep=2):
            event(item, zz, *ways)
            waiting.append((item, zz))
            settle(keep)

        def settle(keep):
            while len(waiting) > keep:
                dot(*waiting.pop(0))

        if bottom:
            for zz in range(1, nz):
                step(KA, zz)
                step(KB, zz)
                if zz == 1:
                    wo_far(1)
            settle(0)
            finish_kv(KA)
            finish_kv(KB)
            for zz in range(nz - 1, 1, -1):
                wo_far(zz)
            for zz in range(1, nz):
                step(WQ, zz, keep=1)
            take_kv(z)
            settle(0)
            finish_q()
            need_kv(z)
            state = attend(None, 0, z)
        elif top:
            step(WQ, 2)
            wo_far(2)
            step(KA, 2)
            step(WQ, 1)
            step(KB, 2)
            step(WQ, 0)
            settle(0)
            finish_q()
            go(query_copy())
            wo_far(1)
            step(KA, 1, keep=1)
            step(KB, 1, keep=1)
            wo_far(0)
            step(KA, 0, keep=1)
            step(KB, 0, keep=1)
            finish_kv(KA)
            settle(0)
            finish_kv(KB)
            take_kv(z)
            need_kv(z)
            peak, total, value = attend(None, 0, z)
            for copy in part_copies(below):
                copy.wait_recv()
            side = jnp.transpose(jnp.broadcast_to(lin[0:1, :], (HD, rows)))[:, 0:1]
            best = jnp.maximum(peak, side)
            near, far = jnp.exp(peak - best), jnp.exp(side - best)
            state = (
                best, total * near + far, value * near + pin[...].astype(jnp.float32) * far
            )
        elif z == 1:
            step(KA, 2, DOWN)
            step(WQ, 0, UP)
            own_send(KB, UP)
            step(KB, 2, DOWN)
            step(KA, 0, UP)
            step(KA, 3, DOWN)
            step(KB, 0, UP)
            step(KB, 3, DOWN)
            own_send(WQ, DOWN)
            settle(0)
            finish_kv(KA)
            finish_kv(KB)
            step(WQ, 2, DOWN)
            step(WQ, 3, DOWN)
            wo_far(0)
            take_kv(z)
            settle(0)
            finish_q()
            need_kv(z)
            state = attend(None, 0, z)
            take_kv(0)
            wo_far(2)
            wo_far(3)
            need_kv(0)
            state = attend(state, 0, 0)
        else:
            step(WQ, 1, UP)
            own_send(KB, UP)
            step(KA, 3, DOWN)
            step(KB, 3, DOWN)
            own_send(WQ, DOWN)
            step(KA, 1)
            step(WQ, 3, DOWN)
            wo_far(1)
            step(WQ, 0, UP)
            go(chain(KA, 1, UP))
            step(KB, 1, UP)
            step(KA, 0, UP)
            wo_far(0)
            step(KB, 0, UP)
            wo_far(3)
            settle(0)
            finish_kv(KA)
            finish_kv(KB)
            finish_q()
            take_kv(1)
            need_kv(1)
            state = attend(None, 0, 1)
            query_copy().wait_recv()
            other = attend(None, 1, 1)
            take_kv(z)
            need_kv(z)
            other = attend(other, 1, z)
            state = attend(state, 0, z)
            take_kv(0)
            need_kv(0)
            peak, total, value = attend(other, 1, 0)
            part[...] = (value / total).astype(jnp.bfloat16)
            lse[...] = jnp.transpose(
                jnp.broadcast_to(peak + jnp.log(total), (rows, HD))
            )[:lse.shape[0], :]
            for copy in part_copies(above):
                go(copy)
            state = attend(state, 0, 0)

        hloc[...] = (state[2] / state[1]).astype(jnp.bfloat16)
        for k in range(1, nt):
            head_copy(k).start()
        head_cols(t)[...] = hloc[...]

        for g in range(nt):
            arrived = remote(woc, wo_block(g, c), wi_ss.at[0], wi_rs.at[g], partner)
            if g == z:
                @pl.when(t != z)
                def _():
                    arrived.wait_recv()
            else:
                arrived.wait_recv()
            go(wo_pass(g, c))
        end_kv()

        @pl.when(t != z)
        def _():
            wo_copy(z, z).wait_send()

        for g in range(nt):
            wo_pass(g, 1 - c).wait_recv()
        for copy in sent:
            copy.wait_send()

    for z in range(nz):
        @pl.when(plane_of == z)
        def _():
            plane(z)

    for k in range(1, nt):
        head_copy(k).wait_send()
        g = (t + k) % nt
        remote(hloc, head_cols(g), h_ss.at[k], h_rs.at[g], partner).wait_recv()
    out_ref[...] = lax.dot_general(
        hcat[...], wof[...], (((1,), (1,)), ((), ())), preferred_element_type=jnp.float32
    ).astype(out_ref.dtype)


def fused_body(nz, nt, hidden_states, resp_lengths, w_query, w_keyval, w_out):
    rows, depth = hidden_states.shape
    nout = w_out.shape[1]
    bf16, f32 = jnp.bfloat16, jnp.float32
    dma = pltpu.SemaphoreType.DMA
    hbm = pl.BlockSpec(memory_space=pltpu.HBM)
    return pl.pallas_call(
        functools.partial(fused_kernel, nz, nt),
        out_shape=jax.ShapeDtypeStruct((rows, 2 * nout), bf16),
        in_specs=[pl.BlockSpec(memory_space=pltpu.SMEM), hbm, hbm, hbm, hbm],
        out_specs=pl.BlockSpec(memory_space=pltpu.VMEM),
        scratch_shapes=[
            pltpu.VMEM((rows, depth), bf16),
            pltpu.VMEM((3, depth, HD), bf16),
            pltpu.VMEM((nout, HD), bf16),
            pltpu.VMEM((2 * nout, nt * HD), bf16),
            pltpu.VMEM((2, rows, HD), bf16),
            pltpu.VMEM((2, nz, 2 * rows, HD), bf16),
            pltpu.VMEM((3, rows, HD), f32),
            pltpu.VMEM((2, rows, HD), bf16),
            pltpu.VMEM((rows, HD), bf16),
            pltpu.VMEM((8, rows), f32),
            pltpu.VMEM((rows, HD), bf16),
            pltpu.VMEM((8, rows), f32),
            pltpu.VMEM((rows, HD), bf16),
            pltpu.VMEM((rows, nt * HD), bf16),
            dma((5,)),
            dma((3, nz, 3)),
            dma((3, nz)),
            dma((3, nz)),
            dma((2, nz)),
            dma((2, nz)),
            dma((2, nz)),
            dma((2, nz)),
            dma((nz,)),
            dma((nt,)),
            dma((nt,)),
            dma((nt,)),
            dma((3,)),
            dma((3,)),
            dma((nt,)),
            dma((nt,)),
        ],
        compiler_params=pltpu.CompilerParams(
            collective_id=0, has_side_effects=True, vmem_limit_bytes=67_000_000
        ),
    )(resp_lengths, hidden_states, w_query, w_keyval, w_out.T)


def per_device(mesh, hidden_states, resp_lengths, w_query, w_keyval, w_out):
    nt = mesh.shape["tp"]
    nz = mesh.shape["dp"] // 2
    args = (hidden_states, resp_lengths, w_query, w_keyval, w_out)
    fits = (
        mesh.shape["dp"] == 2 * nz and nz == nt and nt == 4
        and w_query.shape[1] == HD and w_keyval.shape[1] == 2 * HD
        and w_out.shape[0] == HD and w_query.shape[0] % 64 == 0
    )
    return fused_body(nz, nt, *args) if fits else body(*args)


def solution(mesh):
    return jax.shard_map(
        functools.partial(per_device, mesh),
        mesh=mesh,
        in_specs=(P("dp", None), P(), P("dp", "tp"), P("dp", "tp"), P("tp", "dp")),
        out_specs=P("dp", "tp"),
        check_vma=False,
    )
```

```python
import functools

import jax
import jax.numpy as jnp
from jax import lax
from jax.experimental import pallas as pl
from jax.experimental.pallas import tpu as pltpu
from jax.sharding import PartitionSpec as P

HD = 128


def segment_of(position, resp_ends):
    return jnp.sum(
        (position[:, None] >= resp_ends[None, :]).astype(jnp.int32), axis=1, dtype=jnp.int32
    )


def body(hidden_states, resp_lengths, w_query, w_keyval, w_out):
    token_rows = hidden_states.shape[0]
    head_scale = HD ** (-0.5)
    pieces = (
        lax.all_gather(w_query, "dp", axis=0, tiled=True),
        lax.all_gather(w_keyval, "dp", axis=0, tiled=True),
    )
    query_sum = jnp.dot(hidden_states, pieces[0], preferred_element_type=jnp.float32)
    keyval_sum = jnp.dot(hidden_states, pieces[1], preferred_element_type=jnp.float32)
    query = (query_sum * head_scale).astype(jnp.bfloat16)
    keyval = lax.all_gather(keyval_sum.astype(jnp.bfloat16), "tp", axis=1, tiled=True)
    kv_count = keyval.shape[1] // (2 * HD)
    per_group = lax.axis_size("tp") // kv_count
    kv_head = lax.axis_index("tp") // per_group
    key_head = lax.dynamic_slice_in_dim(keyval, kv_head * HD, HD, 1)
    value_head = lax.dynamic_slice_in_dim(keyval, (kv_count + kv_head) * HD, HD, 1)
    head_pair = jnp.concatenate([key_head, value_head], axis=1)
    resp_ends = jnp.cumsum(resp_lengths, dtype=jnp.int32)
    own_begin = lax.axis_index("dp") * token_rows
    query_pos = own_begin + jnp.arange(token_rows, dtype=jnp.int32)
    query_seg = segment_of(query_pos, resp_ends)
    pieces = lax.all_gather(head_pair, "dp", axis=0, tiled=True)
    largest = jnp.full((token_rows,), -1e30, jnp.float32)
    height = pieces.shape[0]
    key_pos = jnp.arange(height, dtype=jnp.int32)
    key_seg = segment_of(key_pos, resp_ends)
    scores = jnp.dot(query, pieces[:, :HD].T, preferred_element_type=jnp.float32)
    allowed = (
        (query_seg[:, None] == key_seg[None, :])
        & (key_pos[None, :] <= query_pos[:, None])
        & (key_pos[None, :] >= 0)
    )
    newest = jnp.maximum(largest, jnp.max(jnp.where(allowed, scores, jnp.float32(-1e30)), axis=1))
    expw = jnp.where(allowed, jnp.exp(scores - newest[:, None]), jnp.float32(0.0))
    denom = jnp.sum(expw, axis=1)
    numer = jnp.dot(expw.astype(jnp.bfloat16), pieces[:, HD:], preferred_element_type=jnp.float32)
    heads_out = (numer / denom[:, None]).astype(jnp.bfloat16)
    terms = jnp.dot(
        heads_out,
        lax.all_gather(w_out, "dp", axis=1, tiled=True),
        preferred_element_type=jnp.float32,
    )
    summed = lax.psum_scatter(terms.astype(jnp.bfloat16), "tp", scatter_dimension=1, tiled=True)
    return summed


MESH = pl.DeviceIdType.MESH
KA, KB, WQ = range(3)
UP, DOWN, SIDE = range(3)
NEG = -1e30


def fused_kernel(
    nz, nt, lens_hbm, hid_hbm, wq_hbm, wkv_hbm, wo_hbm, out_ref,
    hid, w, woc, wox, wof, kvloc, kvb, acc, qb, part, lse, pin, lin, hloc, hcat,
    loc_sem, ss, rs, prs, kv_ss, kv_rs, kp_ss, kp_rs, wc_ss, wx_ss, wx_rs, wi_ss, wi_rs, wp_ss, wp_rs,
    pt_ss, pt_rs, h_ss, h_rs, lens_ref,
):
    dp = lax.axis_index("dp")
    t = lax.axis_index("tp")
    plane_of, c = dp // 2, dp % 2
    rows = hid.shape[0]
    shard = wq_hbm.shape[0]
    nout = wo_hbm.shape[0]
    own = pl.ds(pl.multiple_of(dp * shard, 64), shard)

    loads = [
        pltpu.make_async_copy(wkv_hbm.at[:, pl.ds(0, HD)], w.at[KA, own], loc_sem.at[KA]),
        pltpu.make_async_copy(wkv_hbm.at[:, pl.ds(HD, HD)], w.at[KB, own], loc_sem.at[KB]),
        pltpu.make_async_copy(wq_hbm, w.at[WQ, own], loc_sem.at[WQ]),
        pltpu.make_async_copy(hid_hbm, hid, loc_sem.at[3]),
        pltpu.make_async_copy(wo_hbm, woc, loc_sem.at[4]),
        pltpu.make_async_copy(lens_hbm, lens_ref, loc_sem.at[5]),
    ]
    for load in loads:
        load.start()

    barrier = pltpu.get_barrier_semaphore()
    partner = {"dp": dp + 1 - 2 * c, "tp": t}
    above, below = {"dp": dp + 2, "tp": t}, {"dp": dp - 2, "tp": t}
    has_up, has_down = plane_of < nz - 1, plane_of > 0
    pl.semaphore_signal(barrier, 1, device_id=partner, device_id_type=MESH)

    @pl.when(has_up)
    def _():
        pl.semaphore_signal(barrier, 1, device_id=above, device_id_type=MESH)

    @pl.when(has_down)
    def _():
        pl.semaphore_signal(barrier, 1, device_id=below, device_id_type=MESH)

    for k in range(1, nt):
        pl.semaphore_signal(
            barrier, 1, device_id={"dp": dp, "tp": (t + k) % nt}, device_id_type=MESH
        )
    pl.semaphore_wait(barrier, nt + has_up.astype(jnp.int32) + has_down.astype(jnp.int32))

    def chunk(item, zz, cc):
        return w.at[item, pl.ds(pl.multiple_of((2 * zz + cc) * shard, 64), shard)]

    def remote(src, dst, send, recv, to):
        return pltpu.make_async_remote_copy(
            src, dst, send, recv, device_id=to, device_id_type=MESH
        )

    def chain(item, zz, way):
        ref = chunk(item, zz, c)
        recv = prs.at[item, zz] if way == SIDE else rs.at[item, zz]
        return remote(ref, ref, ss.at[item, zz, way], recv, (above, below, partner)[way])

    def device(zz, tt):
        return {"dp": 2 * zz + c, "tp": tt}

    half_rows = pl.ds(pl.multiple_of(c * rows, 128), rows)
    other_rows = pl.ds(pl.multiple_of((1 - c) * rows, 128), rows)

    def kv_copy(z, b, zz):
        role = t // (nt // 2)
        return remote(
            kvloc.at[b], kvb.at[role, z, half_rows], kv_ss.at[b, zz], kv_rs.at[role, z],
            device(zz, 2 * (t % (nt // 2)) + b),
        )

    def kv_pass(z, role):
        ref = kvb.at[role, z, half_rows]
        return remote(ref, ref, kp_ss.at[role, z], kp_rs.at[role, z], partner)

    def kv_passed(z, role):
        ref = kvb.at[role, z, other_rows]
        return remote(ref, ref, kp_ss.at[role, z], kp_rs.at[role, z], partner)

    def wo_block(g, cc):
        return wof.at[
            pl.ds(pl.multiple_of(cc * nout, 64), nout), pl.ds(pl.multiple_of(g * HD, HD), HD)
        ]

    def wo_half(g, h):
        start = pl.multiple_of(c * nout + h * (nout // 2), 16)
        return wof.at[pl.ds(start, nout // 2), pl.ds(pl.multiple_of(g * HD, HD), HD)]

    def wo_ref(g, way):
        return wo_half(g, 0) if g == (nt - 1 if way == UP else 0) else wo_block(g, c)

    def wo_chain(g, way):
        ref = wo_ref(g, way)
        return remote(ref, ref, wc_ss.at[g, way], wi_rs.at[g], (above, below)[way])

    def wo_loose(src, zz, way):
        return remote(src, wox.at[zz], wx_ss.at[zz, way], wx_rs.at[zz], (above, below)[way])

    def wo_cross(zz):
        return remote(woc, wo_block(t, c), wi_ss.at[zz], wi_rs.at[t], {"dp": dp, "tp": zz})

    def wo_loose_cross(zz):
        return remote(
            wox.at[zz], wo_half(t, 1), wi_ss.at[zz], wx_rs.at[nz], {"dp": dp, "tp": zz}
        )

    def wo_pass(g, cc):
        ref = wo_block(g, cc)
        return remote(ref, ref, wp_ss.at[g], wp_rs.at[g], partner)

    def head_cols(g):
        return hcat.at[:, pl.ds(pl.multiple_of(g * HD, HD), HD)]

    def head_copy(k):
        return remote(
            hloc, head_cols(t), h_ss.at[k], h_rs.at[t], {"dp": dp, "tp": (t + k) % nt}
        )

    loads[5].wait()
    ends = []
    end = jnp.int32(0)
    for r in range(lens_ref.shape[0]):
        end = end + lens_ref[r]
        ends.append(end)

    def plane(z):
        sent = []
        seen = set()
        top, bottom = z == nz - 1, z == 0
        kv_to = [zz for zz in (nz - 2, nz - 3, 0) if zz >= z] if not top else [z]
        span = 2 * shard

        def go(copy):
            copy.start()
            sent.append(copy)

        def own_send(item, way):
            go(chain(item, z, way))

        def event(item, zz, *ways):
            ref = chunk(item, zz, c)
            remote(ref, ref, ss.at[item, zz, UP], rs.at[item, zz], partner).wait_recv()
            for way in ways + (SIDE,):
                go(chain(item, zz, way))

        def dot(item, zz):
            ref = chunk(item, zz, 1 - c)
            remote(ref, ref, ss.at[item, zz, SIDE], prs.at[item, zz], partner).wait_recv()
            part_sum = jnp.dot(
                hid[:, zz * span:(zz + 1) * span], w[item, zz * span:(zz + 1) * span, :],
                preferred_element_type=jnp.float32,
            )
            if item in seen:
                acc[item] += part_sum
            else:
                seen.add(item)
                acc[item] = part_sum

        def finish_kv(b):
            kvloc[b] = acc[b].astype(jnp.bfloat16)
            role = t // (nt // 2)
            for zz in kv_to:
                if zz != z:
                    go(kv_copy(z, b, zz))
            mine = 2 * (t % (nt // 2)) + b == t

            @pl.when(jnp.logical_not(mine))
            def _():
                kv_copy(z, b, z).start()

            @pl.when(mine)
            def _():
                kvb[role, z, half_rows, :] = kvloc[b]

        def end_kv():
            for b in range(2):
                @pl.when(2 * (t % (nt // 2)) + b != t)
                def _():
                    kv_copy(z, b, z).wait_send()

        def take_kv(zs):
            for role in range(2):
                arrived = remote(
                    kvloc.at[0], kvb.at[role, zs, half_rows], kv_ss.at[0, zs],
                    kv_rs.at[role, zs], partner,
                )
                if zs == z:
                    @pl.when(t // 2 + role * (nt // 2) != t)
                    def _():
                        arrived.wait_recv()
                else:
                    arrived.wait_recv()
                go(kv_pass(zs, role))

        def need_kv(zs):
            for role in range(2):
                kv_passed(zs, role).wait_recv()

        def finish_q():
            qb[0] = (acc[WQ] * (HD ** -0.5)).astype(jnp.bfloat16)

        def attend(state, qi, zs):
            qpos = (dp + 2 * qi) * rows + lax.broadcasted_iota(jnp.int32, (rows, 1), 0)
            first = jnp.zeros((rows, 1), jnp.int32)
            for e in ends:
                first = jnp.where(qpos >= e, e, first)
            s = lax.dot_general(
                qb[qi], kvb[0, zs], (((1,), (1,)), ((), ())), preferred_element_type=jnp.float32
            )
            kpos = zs * 2 * rows + lax.broadcasted_iota(jnp.int32, s.shape, 1)
            s = jnp.where((kpos >= first) & (kpos <= qpos), s, jnp.float32(NEG))
            peak = jnp.max(s, axis=1, keepdims=True)
            if state is not None:
                peak = jnp.maximum(state[0], peak)
            p = jnp.exp(s - peak)
            total = jnp.sum(p, axis=1, keepdims=True)
            value = jnp.dot(
                p.astype(jnp.bfloat16), kvb[1, zs], preferred_element_type=jnp.float32
            )
            if state is not None:
                fade = jnp.exp(state[0] - peak)
                total = total + state[1] * fade
                value = value + state[2] * fade
            return peak, total, value

        last = nt - 1

        def go_if(cond, copy):
            @pl.when(cond)
            def _():
                copy.start()
            sent.append((cond, copy))

        def wo_arrived(g, ref):
            remote(ref, ref, wc_ss.at[g, UP], wi_rs.at[g], partner).wait_recv()

        def collect():
            @pl.when(t == z)
            def _():
                for g in range(nt):
                    if g != z:
                        wo_arrived(g, wo_block(g, c))

        def hub(way, *picks):
            for k in picks:
                go_if(t == z, wo_chain(k if way == UP else (k + 1) % nt, way))

        def loose(way):
            go_if(t == (last if way == UP else 0), wo_loose(woc.at[pl.ds(nout // 2, nout // 2)], z, way))

        def relay(way, *picks):
            if z == (0 if way == UP else nz - 1):
                return
            mine = t < z if way == UP else t > z
            for k in picks:
                g = k if way == UP else (k + 1) % nt

                @pl.when(mine)
                def _():
                    wo_arrived(g, wo_ref(g, way))
                if z != (nz - 1 if way == UP else 0):
                    go_if(mine, wo_chain(g, way))

        def relay_loose(way, zs):
            mine = t == (last if way == UP else 0)

            @pl.when(mine)
            def _():
                ref = wox.at[zs]
                remote(ref, ref, wx_ss.at[zs, way], wx_rs.at[zs], partner).wait_recv()
            if z != (nz - 1 if way == UP else 0):
                go_if(mine, wo_loose(wox.at[zs], zs, way))
            go_if(mine, wo_loose_cross(zs))

        def query_copy():
            return remote(qb.at[0], qb.at[1], pt_ss.at[0], pt_rs.at[0], below)

        def part_copies(to):
            return (
                remote(part, pin, pt_ss.at[1], pt_rs.at[1], to),
                remote(lse, lin, pt_ss.at[2], pt_rs.at[2], to),
            )

        order = (KA, KB, WQ) if top else (WQ, KA, KB)
        for item in order:
            loads[item].wait()
            if not top and (bottom or item != KB):
                own_send(item, UP)
            if top or (not bottom and item != WQ):
                own_send(item, DOWN)
            own_send(item, SIDE)
        loads[4].wait()
        go_if(t != z, wo_cross(z))

        @pl.when(t == z)
        def _():
            wo_block(t, c)[...] = woc[...]

        loads[3].wait()

        waiting = [(WQ, z), (KA, z), (KB, z)]

        def step(item, zz, *ways, keep=2):
            event(item, zz, *ways)
            waiting.append((item, zz))
            settle(keep)

        def settle(keep):
            while len(waiting) > keep:
                dot(*waiting.pop(0))

        if bottom:
            step(KA, 1)
            collect()
            loose(UP)
            hub(UP, 0, 1, 2, 3)
            step(KB, 1)
            for zz in range(2, nz):
                step(KA, zz)
                step(KB, zz)
            settle(0)
            finish_kv(KA)
            finish_kv(KB)
            for zz in range(1, nz):
                step(WQ, zz, keep=1)
            take_kv(z)
            settle(0)
            finish_q()
            need_kv(z)
            state = attend(None, 0, z)
        elif top:
            step(WQ, 2)
            step(KA, 2)
            collect()
            loose(DOWN)
            hub(DOWN, 0, 1, 2, 3)
            step(WQ, 1)
            step(KB, 2)
            step(WQ, 0)
            settle(0)
            finish_q()
            go(query_copy())
            step(KA, 1, keep=1)
            step(KB, 1, keep=1)
            step(KA, 0, keep=1)
            step(KB, 0, keep=1)
            finish_kv(KA)
            settle(0)
            finish_kv(KB)
            take_kv(z)
            need_kv(z)
            peak, total, value = attend(None, 0, z)
            for copy in part_copies(below):
                copy.wait_recv()
            side = jnp.transpose(jnp.broadcast_to(lin[0:1, :], (HD, rows)))[:, 0:1]
            best = jnp.maximum(peak, side)
            near, far = jnp.exp(peak - best), jnp.exp(side - best)
            state = (
                best, total * near + far, value * near + pin[...].astype(jnp.float32) * far
            )
        elif z == 1:
            step(WQ, 0, UP)
            own_send(KB, UP)
            step(KA, 2, DOWN)
            step(KA, 0, UP)
            step(KB, 2, DOWN)
            step(KA, 3, DOWN)
            step(KB, 0, UP)
            step(KB, 3, DOWN)
            own_send(WQ, DOWN)
            collect()
            settle(0)
            finish_kv(KA)
            finish_kv(KB)
            loose(UP)
            hub(UP, 0)
            relay(UP, 0)
            relay_loose(UP, 0)
            step(WQ, 2, DOWN)
            step(WQ, 3, DOWN)
            loose(DOWN)
            hub(DOWN, 0, 1, 2, 3)
            take_kv(z)
            settle(0)
            finish_q()
            need_kv(z)
            state = attend(None, 0, z)
            relay(DOWN, 0, 1)
            relay_loose(DOWN, 2)
            relay_loose(DOWN, 3)
            take_kv(0)
            hub(UP, 1, 2, 3)
            relay(UP, 1, 2, 3)
            relay(DOWN, 2, 3)
            need_kv(0)
            state = attend(state, 0, 0)
        else:
            step(WQ, 1, UP)
            own_send(KB, UP)
            step(KA, 3, DOWN)
            step(KB, 3, DOWN)
            own_send(WQ, DOWN)
            step(KA, 1)
            step(WQ, 3, DOWN)
            step(WQ, 0, UP)
            go(chain(KA, 1, UP))
            collect()
            loose(DOWN)
            hub(DOWN, 0, 1, 2, 3)
            step(KB, 1, UP)
            relay(DOWN, 0)
            relay_loose(DOWN, 3)
            step(KA, 0, UP)
            relay(DOWN, 1)
            step(KB, 0, UP)
            loose(UP)
            hub(UP, 0)
            settle(0)
            finish_kv(KA)
            finish_kv(KB)
            finish_q()
            relay(DOWN, 2, 3)
            take_kv(1)
            need_kv(1)
            state = attend(None, 0, 1)
            query_copy().wait_recv()
            other = attend(None, 1, 1)
            take_kv(z)
            need_kv(z)
            other = attend(other, 1, z)
            state = attend(state, 0, z)
            relay(UP, 0)
            relay_loose(UP, 1)
            take_kv(0)
            need_kv(0)
            peak, total, value = attend(other, 1, 0)
            part[...] = (value / total).astype(jnp.bfloat16)
            lse[...] = jnp.transpose(
                jnp.broadcast_to(peak + jnp.log(total), (rows, HD))
            )[:lse.shape[0], :]
            for copy in part_copies(above):
                go(copy)
            hub(UP, 1, 2, 3)
            relay_loose(UP, 0)
            state = attend(state, 0, 0)

        hloc[...] = (state[2] / state[1]).astype(jnp.bfloat16)
        for k in range(1, nt):
            head_copy(k).start()
        head_cols(t)[...] = hloc[...]

        if bottom:
            for zz in range(1, nz):
                relay_loose(DOWN, zz)
            relay(DOWN, 0, 1, 2, 3)
        elif top:
            for zz in range(nz - 2, -1, -1):
                relay_loose(UP, zz)
            relay(UP, 0, 1, 2, 3)
        elif z == 2:
            relay(UP, 1, 2, 3)

        @pl.when(t != z)
        def _():
            ref = wox.at[0]
            remote(ref, ref, wi_ss.at[z], wx_rs.at[nz], partner).wait_recv()
        for g in range(nt):
            wo_pass(g, c).start()
        end_kv()
        for copy in sent:
            if isinstance(copy, tuple):
                @pl.when(copy[0])
                def _():
                    copy[1].wait_send()
            else:
                copy.wait_send()

    for z in range(nz):
        @pl.when(plane_of == z)
        def _():
            plane(z)

    for g in range(nt):
        wo_pass(g, 1 - c).wait_recv()
    for k in range(1, nt):
        g = (t + k) % nt
        remote(hloc, head_cols(g), h_ss.at[k], h_rs.at[g], partner).wait_recv()
    out_ref[...] = lax.dot_general(
        hcat[...], wof[...], (((1,), (1,)), ((), ())), preferred_element_type=jnp.float32
    ).astype(out_ref.dtype)
    for k in range(1, nt):
        head_copy(k).wait_send()
    for g in range(nt):
        wo_pass(g, c).wait_send()


def fused_body(nz, nt, hidden_states, resp_lengths, w_query, w_keyval, w_out):
    rows, depth = hidden_states.shape
    nout = w_out.shape[1]
    bf16, f32 = jnp.bfloat16, jnp.float32
    dma = pltpu.SemaphoreType.DMA
    hbm = pl.BlockSpec(memory_space=pltpu.HBM)
    return pl.pallas_call(
        functools.partial(fused_kernel, nz, nt),
        out_shape=jax.ShapeDtypeStruct((rows, 2 * nout), bf16),
        in_specs=[hbm] * 5,
        out_specs=pl.BlockSpec(memory_space=pltpu.VMEM),
        scratch_shapes=[
            pltpu.VMEM((rows, depth), bf16),
            pltpu.VMEM((3, depth, HD), bf16),
            pltpu.VMEM((nout, HD), bf16),
            pltpu.VMEM((nz, nout // 2, HD), bf16),
            pltpu.VMEM((2 * nout, nt * HD), bf16),
            pltpu.VMEM((2, rows, HD), bf16),
            pltpu.VMEM((2, nz, 2 * rows, HD), bf16),
            pltpu.VMEM((3, rows, HD), f32),
            pltpu.VMEM((2, rows, HD), bf16),
            pltpu.VMEM((rows, HD), bf16),
            pltpu.VMEM((8, rows), f32),
            pltpu.VMEM((rows, HD), bf16),
            pltpu.VMEM((8, rows), f32),
            pltpu.VMEM((rows, HD), bf16),
            pltpu.VMEM((rows, nt * HD), bf16),
            dma((6,)),
            dma((3, nz, 3)),
            dma((3, nz)),
            dma((3, nz)),
            dma((2, nz)),
            dma((2, nz)),
            dma((2, nz)),
            dma((2, nz)),
            dma((nt, 2)),
            dma((nz, 2)),
            dma((nz + 1,)),
            dma((nz,)),
            dma((nt,)),
            dma((nt,)),
            dma((nt,)),
            dma((3,)),
            dma((3,)),
            dma((nt,)),
            dma((nt,)),
            pltpu.SMEM(resp_lengths.shape, jnp.int32),
        ],
        compiler_params=pltpu.CompilerParams(
            collective_id=0, has_side_effects=True, vmem_limit_bytes=40_000_000
        ),
    )(*[
        pltpu.with_memory_space_constraint(x, pltpu.HBM)
        for x in (resp_lengths, hidden_states, w_query, w_keyval, w_out.T)
    ])


def per_device(mesh, hidden_states, resp_lengths, w_query, w_keyval, w_out):
    nt = mesh.shape["tp"]
    nz = mesh.shape["dp"] // 2
    args = (hidden_states, resp_lengths, w_query, w_keyval, w_out)
    fits = (
        mesh.shape["dp"] == 2 * nz and nz == nt and nt == 4
        and w_query.shape[1] == HD and w_keyval.shape[1] == 2 * HD
        and w_out.shape[0] == HD and w_query.shape[0] % 64 == 0
    )
    return fused_body(nz, nt, *args) if fits else body(*args)


def solution(mesh):
    return jax.shard_map(
        functools.partial(per_device, mesh),
        mesh=mesh,
        in_specs=(P("dp", None), P(), P("dp", "tp"), P("dp", "tp"), P("tp", "dp")),
        out_specs=P("dp", "tp"),
        check_vma=False,
    )
```

```python
import functools

import jax
import jax.numpy as jnp
from jax import lax
from jax.experimental import pallas as pl
from jax.experimental.pallas import tpu as pltpu
from jax.sharding import PartitionSpec as P

HD = 128


def segment_of(position, resp_ends):
    return jnp.sum(
        (position[:, None] >= resp_ends[None, :]).astype(jnp.int32), axis=1, dtype=jnp.int32
    )


def body(hidden_states, resp_lengths, w_query, w_keyval, w_out):
    token_rows = hidden_states.shape[0]
    head_scale = HD ** (-0.5)
    pieces = (
        lax.all_gather(w_query, "dp", axis=0, tiled=True),
        lax.all_gather(w_keyval, "dp", axis=0, tiled=True),
    )
    query_sum = jnp.dot(hidden_states, pieces[0], preferred_element_type=jnp.float32)
    keyval_sum = jnp.dot(hidden_states, pieces[1], preferred_element_type=jnp.float32)
    query = (query_sum * head_scale).astype(jnp.bfloat16)
    keyval = lax.all_gather(keyval_sum.astype(jnp.bfloat16), "tp", axis=1, tiled=True)
    kv_count = keyval.shape[1] // (2 * HD)
    per_group = lax.axis_size("tp") // kv_count
    kv_head = lax.axis_index("tp") // per_group
    key_head = lax.dynamic_slice_in_dim(keyval, kv_head * HD, HD, 1)
    value_head = lax.dynamic_slice_in_dim(keyval, (kv_count + kv_head) * HD, HD, 1)
    head_pair = jnp.concatenate([key_head, value_head], axis=1)
    resp_ends = jnp.cumsum(resp_lengths, dtype=jnp.int32)
    own_begin = lax.axis_index("dp") * token_rows
    query_pos = own_begin + jnp.arange(token_rows, dtype=jnp.int32)
    query_seg = segment_of(query_pos, resp_ends)
    pieces = lax.all_gather(head_pair, "dp", axis=0, tiled=True)
    largest = jnp.full((token_rows,), -1e30, jnp.float32)
    height = pieces.shape[0]
    key_pos = jnp.arange(height, dtype=jnp.int32)
    key_seg = segment_of(key_pos, resp_ends)
    scores = jnp.dot(query, pieces[:, :HD].T, preferred_element_type=jnp.float32)
    allowed = (
        (query_seg[:, None] == key_seg[None, :])
        & (key_pos[None, :] <= query_pos[:, None])
        & (key_pos[None, :] >= 0)
    )
    newest = jnp.maximum(largest, jnp.max(jnp.where(allowed, scores, jnp.float32(-1e30)), axis=1))
    expw = jnp.where(allowed, jnp.exp(scores - newest[:, None]), jnp.float32(0.0))
    denom = jnp.sum(expw, axis=1)
    numer = jnp.dot(expw.astype(jnp.bfloat16), pieces[:, HD:], preferred_element_type=jnp.float32)
    heads_out = (numer / denom[:, None]).astype(jnp.bfloat16)
    terms = jnp.dot(
        heads_out,
        lax.all_gather(w_out, "dp", axis=1, tiled=True),
        preferred_element_type=jnp.float32,
    )
    summed = lax.psum_scatter(terms.astype(jnp.bfloat16), "tp", scatter_dimension=1, tiled=True)
    return summed


MESH = pl.DeviceIdType.MESH
KA, KB, WQ = range(3)
UP, DOWN, SIDE = range(3)
NEG = -1e30
LOOSE = 6


def fused_kernel(
    nz, nt, lens_hbm, hid_hbm, wq_hbm, wkv_hbm, wo_hbm, out_ref,
    hid, w, woc, wox, wof, kvloc, kvb, acc, qb, part, lse, pin, lin, hloc, hcat,
    loc_sem, ss, rs, prs, kv_ss, kv_rs, kp_ss, kp_rs, wc_ss, wx_ss, wx_rs, wi_ss, wi_rs, wp_ss, wp_rs,
    pt_ss, pt_rs, h_ss, h_rs, lens_ref,
):
    dp = lax.axis_index("dp")
    t = lax.axis_index("tp")
    plane_of, c = dp // 2, dp % 2
    rows = hid.shape[0]
    shard = wq_hbm.shape[0]
    nout = wo_hbm.shape[0]
    own = pl.ds(pl.multiple_of(dp * shard, 64), shard)

    loads = [
        pltpu.make_async_copy(wkv_hbm.at[:, pl.ds(0, HD)], w.at[KA, own], loc_sem.at[KA]),
        pltpu.make_async_copy(wkv_hbm.at[:, pl.ds(HD, HD)], w.at[KB, own], loc_sem.at[KB]),
        pltpu.make_async_copy(wq_hbm, w.at[WQ, own], loc_sem.at[WQ]),
        pltpu.make_async_copy(hid_hbm, hid, loc_sem.at[3]),
        pltpu.make_async_copy(wo_hbm, woc, loc_sem.at[4]),
        pltpu.make_async_copy(lens_hbm, lens_ref, loc_sem.at[5]),
    ]
    for load in loads:
        load.start()

    barrier = pltpu.get_barrier_semaphore()
    partner = {"dp": dp + 1 - 2 * c, "tp": t}
    above, below = {"dp": dp + 2, "tp": t}, {"dp": dp - 2, "tp": t}
    has_up, has_down = plane_of < nz - 1, plane_of > 0
    pl.semaphore_signal(barrier, 1, device_id=partner, device_id_type=MESH)

    @pl.when(has_up)
    def _():
        pl.semaphore_signal(barrier, 1, device_id=above, device_id_type=MESH)

    @pl.when(has_down)
    def _():
        pl.semaphore_signal(barrier, 1, device_id=below, device_id_type=MESH)

    for k in range(1, nt):
        pl.semaphore_signal(
            barrier, 1, device_id={"dp": dp, "tp": (t + k) % nt}, device_id_type=MESH
        )
    pl.semaphore_wait(barrier, nt + has_up.astype(jnp.int32) + has_down.astype(jnp.int32))

    def chunk(item, zz, cc):
        return w.at[item, pl.ds(pl.multiple_of((2 * zz + cc) * shard, 64), shard)]

    def remote(src, dst, send, recv, to):
        return pltpu.make_async_remote_copy(
            src, dst, send, recv, device_id=to, device_id_type=MESH
        )

    def chain(item, zz, way):
        ref = chunk(item, zz, c)
        recv = prs.at[item, zz] if way == SIDE else rs.at[item, zz]
        return remote(ref, ref, ss.at[item, zz, way], recv, (above, below, partner)[way])

    def device(zz, tt):
        return {"dp": 2 * zz + c, "tp": tt}

    half_rows = pl.ds(pl.multiple_of(c * rows, 128), rows)
    other_rows = pl.ds(pl.multiple_of((1 - c) * rows, 128), rows)

    def kv_copy(z, b, zz):
        role = t // (nt // 2)
        return remote(
            kvloc.at[b], kvb.at[role, z, half_rows], kv_ss.at[b, zz], kv_rs.at[role, z],
            device(zz, 2 * (t % (nt // 2)) + b),
        )

    def kv_pass(z, role):
        ref = kvb.at[role, z, half_rows]
        return remote(ref, ref, kp_ss.at[role, z], kp_rs.at[role, z], partner)

    def kv_passed(z, role):
        ref = kvb.at[role, z, other_rows]
        return remote(ref, ref, kp_ss.at[role, z], kp_rs.at[role, z], partner)

    def wo_block(g, cc):
        return wof.at[
            pl.ds(pl.multiple_of(cc * nout, 64), nout), pl.ds(pl.multiple_of(g * HD, HD), HD)
        ]

    split = nout - wox.shape[1]

    def wo_half(g, h):
        start = pl.multiple_of(c * nout + h * split, 16)
        size = nout - split if h else split
        return wof.at[pl.ds(start, size), pl.ds(pl.multiple_of(g * HD, HD), HD)]

    def wo_ref(g, way):
        return wo_half(g, 0) if g == (nt - 1 if way == UP else 0) else wo_block(g, c)

    def wo_chain(g, way):
        ref = wo_ref(g, way)
        return remote(ref, ref, wc_ss.at[g, way], wi_rs.at[g], (above, below)[way])

    def wo_loose(src, zz, way):
        return remote(src, wox.at[zz], wx_ss.at[zz, way], wx_rs.at[zz], (above, below)[way])

    def wo_cross(zz):
        return remote(woc, wo_block(t, c), wi_ss.at[zz], wi_rs.at[t], {"dp": dp, "tp": zz})

    def wo_loose_cross(zz):
        return remote(
            wox.at[zz], wo_half(t, 1), wi_ss.at[zz], wx_rs.at[nz], {"dp": dp, "tp": zz}
        )

    def wo_pass(g, cc):
        ref = wo_block(g, cc)
        return remote(ref, ref, wp_ss.at[g], wp_rs.at[g], partner)

    def head_cols(g):
        return hcat.at[:, pl.ds(pl.multiple_of(g * HD, HD), HD)]

    def head_copy(k):
        return remote(
            hloc, head_cols(t), h_ss.at[k], h_rs.at[t], {"dp": dp, "tp": (t + k) % nt}
        )

    loads[5].wait()
    ends = []
    end = jnp.int32(0)
    for r in range(lens_ref.shape[0]):
        end = end + lens_ref[r]
        ends.append(end)

    def plane(z):
        sent = []
        seen = set()
        top, bottom = z == nz - 1, z == 0
        kv_to = [zz for zz in (nz - 2, nz - 3, 0) if zz >= z] if not top else [z]
        span = 2 * shard

        def go(copy):
            copy.start()
            sent.append(copy)

        def own_send(item, way):
            go(chain(item, z, way))

        def event(item, zz, *ways):
            ref = chunk(item, zz, c)
            remote(ref, ref, ss.at[item, zz, UP], rs.at[item, zz], partner).wait_recv()
            for way in ways + (SIDE,):
                go(chain(item, zz, way))

        def dot(item, zz):
            ref = chunk(item, zz, 1 - c)
            remote(ref, ref, ss.at[item, zz, SIDE], prs.at[item, zz], partner).wait_recv()
            part_sum = jnp.dot(
                hid[:, zz * span:(zz + 1) * span], w[item, zz * span:(zz + 1) * span, :],
                preferred_element_type=jnp.float32,
            )
            if item in seen:
                acc[item] += part_sum
            else:
                seen.add(item)
                acc[item] = part_sum

        def finish_kv(b):
            kvloc[b] = acc[b].astype(jnp.bfloat16)
            role = t // (nt // 2)
            for zz in kv_to:
                if zz != z:
                    go(kv_copy(z, b, zz))
            mine = 2 * (t % (nt // 2)) + b == t

            @pl.when(jnp.logical_not(mine))
            def _():
                kv_copy(z, b, z).start()

            @pl.when(mine)
            def _():
                kvb[role, z, half_rows, :] = kvloc[b]

        def end_kv():
            for b in range(2):
                @pl.when(2 * (t % (nt // 2)) + b != t)
                def _():
                    kv_copy(z, b, z).wait_send()

        def take_kv(zs):
            for role in range(2):
                arrived = remote(
                    kvloc.at[0], kvb.at[role, zs, half_rows], kv_ss.at[0, zs],
                    kv_rs.at[role, zs], partner,
                )
                if zs == z:
                    @pl.when(t // 2 + role * (nt // 2) != t)
                    def _():
                        arrived.wait_recv()
                else:
                    arrived.wait_recv()
                go(kv_pass(zs, role))

        def need_kv(zs):
            for role in range(2):
                kv_passed(zs, role).wait_recv()

        def finish_q():
            qb[0] = (acc[WQ] * (HD ** -0.5)).astype(jnp.bfloat16)

        def attend(state, qi, zs):
            qpos = (dp + 2 * qi) * rows + lax.broadcasted_iota(jnp.int32, (rows, 1), 0)
            first = jnp.zeros((rows, 1), jnp.int32)
            for e in ends:
                first = jnp.where(qpos >= e, e, first)
            s = lax.dot_general(
                qb[qi], kvb[0, zs], (((1,), (1,)), ((), ())), preferred_element_type=jnp.float32
            )
            kpos = zs * 2 * rows + lax.broadcasted_iota(jnp.int32, s.shape, 1)
            s = jnp.where((kpos >= first) & (kpos <= qpos), s, jnp.float32(NEG))
            peak = jnp.max(s, axis=1, keepdims=True)
            if state is not None:
                peak = jnp.maximum(state[0], peak)
            p = jnp.exp(s - peak)
            total = jnp.sum(p, axis=1, keepdims=True)
            value = jnp.dot(
                p.astype(jnp.bfloat16), kvb[1, zs], preferred_element_type=jnp.float32
            )
            if state is not None:
                fade = jnp.exp(state[0] - peak)
                total = total + state[1] * fade
                value = value + state[2] * fade
            return peak, total, value

        last = nt - 1

        def go_if(cond, copy):
            @pl.when(cond)
            def _():
                copy.start()
            sent.append((cond, copy))

        def wo_arrived(g, ref):
            remote(ref, ref, wc_ss.at[g, UP], wi_rs.at[g], partner).wait_recv()

        def collect():
            @pl.when(t == z)
            def _():
                for g in range(nt):
                    if g != z:
                        wo_arrived(g, wo_block(g, c))

        def hub(way, *picks):
            for k in picks:
                go_if(t == z, wo_chain(k if way == UP else (k + 1) % nt, way))

        def loose(way):
            go_if(t == (last if way == UP else 0), wo_loose(woc.at[pl.ds(split, nout - split)], z, way))

        def relay(way, *picks):
            if z == (0 if way == UP else nz - 1):
                return
            mine = t < z if way == UP else t > z
            for k in picks:
                g = k if way == UP else (k + 1) % nt

                @pl.when(mine)
                def _():
                    wo_arrived(g, wo_ref(g, way))
                if z != (nz - 1 if way == UP else 0):
                    go_if(mine, wo_chain(g, way))

        def relay_loose(way, zs):
            mine = t == (last if way == UP else 0)

            @pl.when(mine)
            def _():
                ref = wox.at[zs]
                remote(ref, ref, wx_ss.at[zs, way], wx_rs.at[zs], partner).wait_recv()
            if z != (nz - 1 if way == UP else 0):
                go_if(mine, wo_loose(wox.at[zs], zs, way))
            go_if(mine, wo_loose_cross(zs))

        def query_copy():
            return remote(qb.at[0], qb.at[1], pt_ss.at[0], pt_rs.at[0], below)

        def part_copies(to):
            return (
                remote(part, pin, pt_ss.at[1], pt_rs.at[1], to),
                remote(lse, lin, pt_ss.at[2], pt_rs.at[2], to),
            )

        order = (KA, KB, WQ) if top else (WQ, KA, KB)
        for item in order:
            loads[item].wait()
            if not top and (bottom or item != KB):
                own_send(item, UP)
            if top or (not bottom and item != WQ):
                own_send(item, DOWN)
            own_send(item, SIDE)
        loads[4].wait()
        go_if(t != z, wo_cross(z))

        @pl.when(t == z)
        def _():
            wo_block(t, c)[...] = woc[...]

        loads[3].wait()

        waiting = [(WQ, z), (KA, z), (KB, z)]

        def step(item, zz, *ways, keep=2):
            event(item, zz, *ways)
            waiting.append((item, zz))
            settle(keep)

        def settle(keep):
            while len(waiting) > keep:
                dot(*waiting.pop(0))

        if bottom:
            step(KA, 1)
            collect()
            loose(UP)
            hub(UP, 0, 1, 2, 3)
            step(KB, 1)
            for zz in range(2, nz):
                step(KA, zz)
                step(KB, zz)
            settle(0)
            finish_kv(KA)
            finish_kv(KB)
            for zz in range(1, nz):
                step(WQ, zz, keep=1)
            take_kv(z)
            settle(0)
            finish_q()
            need_kv(z)
            state = attend(None, 0, z)
        elif top:
            step(WQ, 2)
            step(KA, 2)
            collect()
            loose(DOWN)
            hub(DOWN, 0, 1, 2, 3)
            step(WQ, 1)
            step(KB, 2)
            step(WQ, 0)
            settle(0)
            finish_q()
            go(query_copy())
            step(KA, 1, keep=1)
            step(KB, 1, keep=1)
            step(KA, 0, keep=1)
            step(KB, 0, keep=1)
            finish_kv(KA)
            settle(0)
            finish_kv(KB)
            take_kv(z)
            need_kv(z)
            peak, total, value = attend(None, 0, z)
            for zz in range(nz - 2, -1, -1):
                relay_loose(UP, zz)
            for copy in part_copies(below):
                copy.wait_recv()
            side = jnp.transpose(jnp.broadcast_to(lin[0:1, :], (HD, rows)))[:, 0:1]
            best = jnp.maximum(peak, side)
            near, far = jnp.exp(peak - best), jnp.exp(side - best)
            state = (
                best, total * near + far, value * near + pin[...].astype(jnp.float32) * far
            )
        elif z == 1:
            step(WQ, 0, UP)
            own_send(KB, UP)
            step(KA, 2, DOWN)
            step(KA, 0, UP)
            step(KB, 2, DOWN)
            step(KA, 3, DOWN)
            step(KB, 0, UP)
            step(KB, 3, DOWN)
            own_send(WQ, DOWN)
            collect()
            settle(0)
            finish_kv(KA)
            finish_kv(KB)
            loose(UP)
            hub(UP, 0, 1, 2, 3)
            relay(UP, 0, 1, 2, 3)
            relay_loose(UP, 0)
            step(WQ, 2, DOWN)
            step(WQ, 3, DOWN)
            loose(DOWN)
            hub(DOWN, 0, 1, 2, 3)
            take_kv(z)
            settle(0)
            finish_q()
            need_kv(z)
            state = attend(None, 0, z)
            relay(DOWN, 0, 1)
            relay_loose(DOWN, 2)
            relay_loose(DOWN, 3)
            take_kv(0)
            relay(DOWN, 2, 3)
            need_kv(0)
            state = attend(state, 0, 0)
        else:
            step(WQ, 1, UP)
            own_send(KB, UP)
            step(KA, 3, DOWN)
            step(KB, 3, DOWN)
            own_send(WQ, DOWN)
            step(KA, 1)
            step(WQ, 3, DOWN)
            step(WQ, 0, UP)
            go(chain(KA, 1, UP))
            collect()
            loose(DOWN)
            hub(DOWN, 0, 1, 2, 3)
            step(KB, 1, UP)
            relay(DOWN, 0)
            relay_loose(DOWN, 3)
            step(KA, 0, UP)
            relay(DOWN, 1)
            step(KB, 0, UP)
            loose(UP)
            hub(UP, 0)
            settle(0)
            finish_kv(KA)
            finish_kv(KB)
            finish_q()
            relay(DOWN, 2, 3)
            take_kv(1)
            need_kv(1)
            state = attend(None, 0, 1)
            query_copy().wait_recv()
            other = attend(None, 1, 1)
            take_kv(z)
            need_kv(z)
            other = attend(other, 1, z)
            state = attend(state, 0, z)
            relay(UP, 0)
            relay_loose(UP, 1)
            relay_loose(UP, 0)
            take_kv(0)
            need_kv(0)
            relay(UP, 1)
            peak, total, value = attend(other, 1, 0)
            part[...] = (value / total).astype(jnp.bfloat16)
            lse[...] = jnp.transpose(
                jnp.broadcast_to(peak + jnp.log(total), (rows, HD))
            )[:lse.shape[0], :]
            for copy in part_copies(above):
                go(copy)
            hub(UP, 1, 2, 3)
            state = attend(state, 0, 0)

        hloc[...] = (state[2] / state[1]).astype(jnp.bfloat16)
        for k in range(1, nt):
            head_copy(k).start()
        head_cols(t)[...] = hloc[...]

        if bottom:
            for zz in range(1, nz):
                relay_loose(DOWN, zz)
            relay(DOWN, 0, 1, 2, 3)
        elif top:
            relay(UP, 0, 1, 2, 3)
        elif z == 2:
            relay(UP, 2, 3)

        @pl.when(t != z)
        def _():
            ref = wox.at[0]
            remote(ref, ref, wi_ss.at[z], wx_rs.at[nz], partner).wait_recv()
        for g in range(nt):
            wo_pass(g, c).start()
        for g in range(nt):
            wo_pass(g, 1 - c).wait_recv()
        for k in range(1, nt):
            g = (t + k) % nt
            remote(hloc, head_cols(g), h_ss.at[k], h_rs.at[g], partner).wait_recv()
        out_ref[...] = lax.dot_general(
            hcat[...], wof[...], (((1,), (1,)), ((), ())), preferred_element_type=jnp.float32
        ).astype(out_ref.dtype)
        for k in range(1, nt):
            head_copy(k).wait_send()
        for g in range(nt):
            wo_pass(g, c).wait_send()
        end_kv()
        for copy in sent:
            if isinstance(copy, tuple):
                @pl.when(copy[0])
                def _():
                    copy[1].wait_send()
            else:
                copy.wait_send()

    for z in range(nz):
        @pl.when(plane_of == z)
        def _():
            plane(z)


def fused_body(nz, nt, hidden_states, resp_lengths, w_query, w_keyval, w_out):
    rows, depth = hidden_states.shape
    nout = w_out.shape[1]
    bf16, f32 = jnp.bfloat16, jnp.float32
    dma = pltpu.SemaphoreType.DMA
    hbm = pl.BlockSpec(memory_space=pltpu.HBM)
    return pl.pallas_call(
        functools.partial(fused_kernel, nz, nt),
        out_shape=jax.ShapeDtypeStruct((rows, 2 * nout), bf16),
        in_specs=[hbm] * 5,
        out_specs=pl.BlockSpec(memory_space=pltpu.VMEM),
        scratch_shapes=[
            pltpu.VMEM((rows, depth), bf16),
            pltpu.VMEM((3, depth, HD), bf16),
            pltpu.VMEM((nout, HD), bf16),
            pltpu.VMEM((nz, nout * LOOSE // 8, HD), bf16),
            pltpu.VMEM((2 * nout, nt * HD), bf16),
            pltpu.VMEM((2, rows, HD), bf16),
            pltpu.VMEM((2, nz, 2 * rows, HD), bf16),
            pltpu.VMEM((3, rows, HD), f32),
            pltpu.VMEM((2, rows, HD), bf16),
            pltpu.VMEM((rows, HD), bf16),
            pltpu.VMEM((8, rows), f32),
            pltpu.VMEM((rows, HD), bf16),
            pltpu.VMEM((8, rows), f32),
            pltpu.VMEM((rows, HD), bf16),
            pltpu.VMEM((rows, nt * HD), bf16),
            dma((6,)),
            dma((3, nz, 3)),
            dma((3, nz)),
            dma((3, nz)),
            dma((2, nz)),
            dma((2, nz)),
            dma((2, nz)),
            dma((2, nz)),
            dma((nt, 2)),
            dma((nz, 2)),
            dma((nz + 1,)),
            dma((nz,)),
            dma((nt,)),
            dma((nt,)),
            dma((nt,)),
            dma((3,)),
            dma((3,)),
            dma((nt,)),
            dma((nt,)),
            pltpu.SMEM(resp_lengths.shape, jnp.int32),
        ],
        compiler_params=pltpu.CompilerParams(
            collective_id=0, has_side_effects=True, vmem_limit_bytes=40_000_000
        ),
    )(*[
        pltpu.with_memory_space_constraint(x, pltpu.HBM)
        for x in (resp_lengths, hidden_states, w_query, w_keyval, w_out.T)
    ])


def per_device(mesh, hidden_states, resp_lengths, w_query, w_keyval, w_out):
    nt = mesh.shape["tp"]
    nz = mesh.shape["dp"] // 2
    args = (hidden_states, resp_lengths, w_query, w_keyval, w_out)
    fits = (
        mesh.shape["dp"] == 2 * nz and nz == nt and nt == 4
        and w_query.shape[1] == HD and w_keyval.shape[1] == 2 * HD
        and w_out.shape[0] == HD and w_query.shape[0] % 64 == 0
    )
    return fused_body(nz, nt, *args) if fits else body(*args)


def solution(mesh):
    return jax.shard_map(
        functools.partial(per_device, mesh),
        mesh=mesh,
        in_specs=(P("dp", None), P(), P("dp", "tp"), P("dp", "tp"), P("tp", "dp")),
        out_specs=P("dp", "tp"),
        check_vma=False,
    )
```

```python
import functools

import jax
import jax.numpy as jnp
from jax import lax
from jax.experimental import pallas as pl
from jax.experimental.pallas import tpu as pltpu
from jax.sharding import PartitionSpec as P

HD = 128


def segment_of(position, resp_ends):
    return jnp.sum(
        (position[:, None] >= resp_ends[None, :]).astype(jnp.int32), axis=1, dtype=jnp.int32
    )


def body(hidden_states, resp_lengths, w_query, w_keyval, w_out):
    token_rows = hidden_states.shape[0]
    head_scale = HD ** (-0.5)
    pieces = (
        lax.all_gather(w_query, "dp", axis=0, tiled=True),
        lax.all_gather(w_keyval, "dp", axis=0, tiled=True),
    )
    query_sum = jnp.dot(hidden_states, pieces[0], preferred_element_type=jnp.float32)
    keyval_sum = jnp.dot(hidden_states, pieces[1], preferred_element_type=jnp.float32)
    query = (query_sum * head_scale).astype(jnp.bfloat16)
    keyval = lax.all_gather(keyval_sum.astype(jnp.bfloat16), "tp", axis=1, tiled=True)
    kv_count = keyval.shape[1] // (2 * HD)
    per_group = lax.axis_size("tp") // kv_count
    kv_head = lax.axis_index("tp") // per_group
    key_head = lax.dynamic_slice_in_dim(keyval, kv_head * HD, HD, 1)
    value_head = lax.dynamic_slice_in_dim(keyval, (kv_count + kv_head) * HD, HD, 1)
    head_pair = jnp.concatenate([key_head, value_head], axis=1)
    resp_ends = jnp.cumsum(resp_lengths, dtype=jnp.int32)
    own_begin = lax.axis_index("dp") * token_rows
    query_pos = own_begin + jnp.arange(token_rows, dtype=jnp.int32)
    query_seg = segment_of(query_pos, resp_ends)
    pieces = lax.all_gather(head_pair, "dp", axis=0, tiled=True)
    largest = jnp.full((token_rows,), -1e30, jnp.float32)
    height = pieces.shape[0]
    key_pos = jnp.arange(height, dtype=jnp.int32)
    key_seg = segment_of(key_pos, resp_ends)
    scores = jnp.dot(query, pieces[:, :HD].T, preferred_element_type=jnp.float32)
    allowed = (
        (query_seg[:, None] == key_seg[None, :])
        & (key_pos[None, :] <= query_pos[:, None])
        & (key_pos[None, :] >= 0)
    )
    newest = jnp.maximum(largest, jnp.max(jnp.where(allowed, scores, jnp.float32(-1e30)), axis=1))
    expw = jnp.where(allowed, jnp.exp(scores - newest[:, None]), jnp.float32(0.0))
    denom = jnp.sum(expw, axis=1)
    numer = jnp.dot(expw.astype(jnp.bfloat16), pieces[:, HD:], preferred_element_type=jnp.float32)
    heads_out = (numer / denom[:, None]).astype(jnp.bfloat16)
    terms = jnp.dot(
        heads_out,
        lax.all_gather(w_out, "dp", axis=1, tiled=True),
        preferred_element_type=jnp.float32,
    )
    summed = lax.psum_scatter(terms.astype(jnp.bfloat16), "tp", scatter_dimension=1, tiled=True)
    return summed


MESH = pl.DeviceIdType.MESH
KA, KB, WQ = range(3)
UP, DOWN, SIDE = range(3)
NEG = -1e30
LOOSE = 6


def fused_kernel(
    nz, nt, lens_hbm, hid_hbm, wq_hbm, wkv_hbm, wo_hbm, out_ref,
    hid, w, woc, wox, wof, kvloc, kvb, acc, qb, part, lse, pin, lin, hloc, hcat,
    loc_sem, ss, rs, prs, kv_ss, kv_rs, kp_ss, kp_rs, wc_ss, wx_ss, wx_rs, wi_ss, wi_rs, wp_ss, wp_rs,
    pt_ss, pt_rs, h_ss, h_rs, lens_ref,
):
    dp = lax.axis_index("dp")
    t = lax.axis_index("tp")
    plane_of, c = dp // 2, dp % 2
    rows = hid.shape[0]
    shard = wq_hbm.shape[0]
    nout = wo_hbm.shape[0]
    own = pl.ds(pl.multiple_of(dp * shard, 64), shard)

    barrier = pltpu.get_barrier_semaphore()
    partner = {"dp": dp + 1 - 2 * c, "tp": t}
    above, below = {"dp": dp + 2, "tp": t}, {"dp": dp - 2, "tp": t}
    has_up, has_down = plane_of < nz - 1, plane_of > 0
    pl.semaphore_signal(barrier, 1, device_id=partner, device_id_type=MESH)

    @pl.when(has_up)
    def _():
        pl.semaphore_signal(barrier, 1, device_id=above, device_id_type=MESH)

    @pl.when(has_down)
    def _():
        pl.semaphore_signal(barrier, 1, device_id=below, device_id_type=MESH)

    for k in range(1, nt):
        pl.semaphore_signal(
            barrier, 1, device_id={"dp": dp, "tp": (t + k) % nt}, device_id_type=MESH
        )
    loads = [
        pltpu.make_async_copy(wkv_hbm.at[:, pl.ds(0, HD)], w.at[KA, own], loc_sem.at[KA]),
        pltpu.make_async_copy(wkv_hbm.at[:, pl.ds(HD, HD)], w.at[KB, own], loc_sem.at[KB]),
        pltpu.make_async_copy(wq_hbm, w.at[WQ, own], loc_sem.at[WQ]),
        pltpu.make_async_copy(hid_hbm, hid, loc_sem.at[3]),
        pltpu.make_async_copy(wo_hbm, woc, loc_sem.at[4]),
        pltpu.make_async_copy(lens_hbm, lens_ref, loc_sem.at[5]),
    ]
    for load in loads:
        load.start()

    pl.semaphore_wait(barrier, nt + has_up.astype(jnp.int32) + has_down.astype(jnp.int32))

    def chunk(item, zz, cc):
        return w.at[item, pl.ds(pl.multiple_of((2 * zz + cc) * shard, 64), shard)]

    def remote(src, dst, send, recv, to):
        return pltpu.make_async_remote_copy(
            src, dst, send, recv, device_id=to, device_id_type=MESH
        )

    def chain(item, zz, way):
        ref = chunk(item, zz, c)
        recv = prs.at[item, zz] if way == SIDE else rs.at[item, zz]
        return remote(
            ref, ref, ss.at[int(item == WQ), way], recv, (above, below, partner)[way]
        )

    def device(zz, tt):
        return {"dp": 2 * zz + c, "tp": tt}

    half_rows = pl.ds(pl.multiple_of(c * rows, 128), rows)
    other_rows = pl.ds(pl.multiple_of((1 - c) * rows, 128), rows)

    def kv_copy(z, b, zz):
        role = t // (nt // 2)
        return remote(
            kvloc.at[b], kvb.at[role, z, half_rows], kv_ss.at[int(zz == z)], kv_rs.at[z],
            device(zz, 2 * (t % (nt // 2)) + b),
        )

    def kv_over(z, b):
        role = t // (nt // 2)
        return remote(
            kvloc.at[b], kvb.at[role, z, pl.ds(0, rows)], kp_ss.at[0], kp_rs.at[z],
            {"dp": dp + 1, "tp": 2 * (t % (nt // 2)) + b},
        )

    def kv_pass(z, role):
        ref = kvb.at[role, z, half_rows]
        return remote(ref, ref, kp_ss.at[0], kp_rs.at[z], partner)

    def wo_block(g, cc):
        return wof.at[
            pl.ds(pl.multiple_of(cc * nout, 64), nout), pl.ds(pl.multiple_of(g * HD, HD), HD)
        ]

    split = nout - wox.shape[1]

    def wo_half(g, h):
        start = pl.multiple_of(c * nout + h * split, 16)
        size = nout - split if h else split
        return wof.at[pl.ds(start, size), pl.ds(pl.multiple_of(g * HD, HD), HD)]

    def wo_ref(g, way):
        return wo_half(g, 0) if g == (nt - 1 if way == UP else 0) else wo_block(g, c)

    def wo_chain(g, way):
        ref = wo_ref(g, way)
        full = int(g != (nt - 1 if way == UP else 0))
        return remote(ref, ref, wc_ss.at[full, way], wi_rs.at[g], (above, below)[way])

    def wo_loose(src, zz, way):
        return remote(src, wox.at[zz], wx_ss.at[way], wx_rs.at[zz], (above, below)[way])

    def wo_cross(zz):
        return remote(woc, wo_block(t, c), wi_ss.at[0], wi_rs.at[t], {"dp": dp, "tp": zz})

    def wo_loose_cross(zz):
        return remote(
            wox.at[zz], wo_half(t, 1), wi_ss.at[1], wx_rs.at[nz], {"dp": dp, "tp": zz}
        )

    def wo_pass(g, cc):
        ref = wo_block(g, cc)
        return remote(ref, ref, wp_ss.at[0], wp_rs.at[0], partner)

    def head_cols(g):
        return hcat.at[:, pl.ds(pl.multiple_of(g * HD, HD), HD)]

    def head_copy(k):
        return remote(
            hloc, head_cols(t), h_ss.at[0], h_rs.at[0], {"dp": dp, "tp": (t + k) % nt}
        )

    loads[5].wait()
    ends = []
    end = jnp.int32(0)
    for r in range(lens_ref.shape[0]):
        end = end + lens_ref[r]
        ends.append(end)

    def plane(z):
        counts = {}
        seen = set()
        top, bottom = z == nz - 1, z == 0
        kv_to = [zz for zz in (nz - 2, nz - 3, 0) if zz >= z] if not top else [z]
        span = 2 * shard

        def tally(key, rows_sent, cond=None):
            counts[key] = (counts.get(key, (0, cond))[0] + rows_sent, cond)

        def go(copy, key, rows_sent):
            copy.start()
            tally(key, rows_sent)

        def go_chain(item, zz, way):
            go(chain(item, zz, way), ("w", int(item == WQ), way), shard)

        def received(ref, sem):
            remote(ref, ref, sem, sem, partner).wait_recv()

        def drain(sem, amount):
            ref = w.at[0, pl.ds(0, amount)]
            remote(ref, ref, sem, sem, partner).wait_send()

        def own_send(item, way):
            go_chain(item, z, way)

        def event(item, zz, *ways):
            ref = chunk(item, zz, c)
            received(ref, rs.at[item, zz])
            for way in ways + (SIDE,):
                go_chain(item, zz, way)

        def dot(item, zz):
            ref = chunk(item, zz, 1 - c)
            received(ref, prs.at[item, zz])
            part_sum = jnp.dot(
                hid[:, zz * span:(zz + 1) * span], w[item, zz * span:(zz + 1) * span, :],
                preferred_element_type=jnp.float32,
            )
            if item in seen:
                acc[item] += part_sum
            else:
                seen.add(item)
                acc[item] = part_sum

        def finish_kv(*picks):
            role = t // (nt // 2)
            for b in picks:
                kvloc[b] = acc[b].astype(jnp.bfloat16)
            for zz in kv_to:
                if zz != z:
                    for b in picks:
                        go(kv_copy(z, b, zz), ("far",), rows)
            for b in picks:
                mine = 2 * (t % (nt // 2)) + b == t
                if top:
                    go_if(c == 0, kv_over(z, b), ("pass",), rows)

                @pl.when(jnp.logical_not(mine))
                def _():
                    kv_copy(z, b, z).start()

                @pl.when(mine)
                def _():
                    kvb[role, z, half_rows, :] = kvloc[b]

        k_here, v_here = t // 2 == t, t // 2 + nt // 2 == t
        none_here = jnp.logical_not(jnp.logical_or(k_here, v_here))

        def end_kv():
            @pl.when(none_here)
            def _():
                drain(kv_ss.at[1], 2 * rows)

            @pl.when(jnp.logical_not(none_here))
            def _():
                drain(kv_ss.at[1], rows)

        def take_kv(zs):
            both = kvb.at[:, zs, half_rows]
            if zs == z:
                @pl.when(none_here)
                def _():
                    received(both, kv_rs.at[zs])

                @pl.when(jnp.logical_not(none_here))
                def _():
                    received(kvb.at[jnp.where(k_here, 1, 0), zs, half_rows], kv_rs.at[zs])
            else:
                received(both, kv_rs.at[zs])
            if not top:
                for role in range(2):
                    go(kv_pass(zs, role), ("pass",), rows)

        def need_kv(zs):
            both = kvb.at[:, zs, other_rows]
            if top:
                @pl.when(c == 1)
                def _():
                    received(both, kp_rs.at[zs])
            else:
                received(both, kp_rs.at[zs])

        def finish_q():
            qb[0] = (acc[WQ] * (HD ** -0.5)).astype(jnp.bfloat16)

        def attend(state, qi, zs):
            qpos = (dp + 2 * qi) * rows + lax.broadcasted_iota(jnp.int32, (rows, 1), 0)
            first = jnp.zeros((rows, 1), jnp.int32)
            for e in ends:
                first = jnp.where(qpos >= e, e, first)
            s = lax.dot_general(
                qb[qi], kvb[0, zs], (((1,), (1,)), ((), ())), preferred_element_type=jnp.float32
            )
            kpos = zs * 2 * rows + lax.broadcasted_iota(jnp.int32, s.shape, 1)
            s = jnp.where((kpos >= first) & (kpos <= qpos), s, jnp.float32(NEG))
            peak = jnp.max(s, axis=1, keepdims=True)
            if state is not None:
                peak = jnp.maximum(state[0], peak)
            p = jnp.exp(s - peak)
            total = jnp.sum(p, axis=1, keepdims=True)
            value = jnp.dot(
                p.astype(jnp.bfloat16), kvb[1, zs], preferred_element_type=jnp.float32
            )
            if state is not None:
                fade = jnp.exp(state[0] - peak)
                total = total + state[1] * fade
                value = value + state[2] * fade
            return peak, total, value

        last = nt - 1

        def go_if(cond, copy, key, rows_sent):
            @pl.when(cond)
            def _():
                copy.start()
            tally(key, rows_sent, cond)

        def wo_arrived(g, ref):
            received(ref, wi_rs.at[g])

        def collect():
            @pl.when(t == z)
            def _():
                for g in range(nt):
                    if g != z:
                        wo_arrived(g, wo_block(g, c))
                    wo_pass(g, c).start()

        def hub(way, *picks):
            for k in picks:
                @pl.when(t == z)
                def _():
                    wo_chain(k if way == UP else (k + 1) % nt, way).start()

        def loose(way):
            go_if(
                t == (last if way == UP else 0),
                wo_loose(woc.at[pl.ds(split, nout - split)], z, way), ("x", way), nout - split,
            )

        def relay(way, *picks, only=None):
            if z == (0 if way == UP else nz - 1):
                return
            mine = t < z if way == UP else t > z
            if only is not None:
                mine = t == only
            for k in picks:
                g = k if way == UP else (k + 1) % nt

                @pl.when(mine)
                def _():
                    wo_arrived(g, wo_ref(g, way))
                    if z != (nz - 1 if way == UP else 0):
                        wo_chain(g, way).start()
                    if k < nt - 1:
                        wo_pass(g, c).start()

        def relay_loose(way, zs):
            mine = t == (last if way == UP else 0)

            @pl.when(mine)
            def _():
                received(wox.at[zs], wx_rs.at[zs])
            if z != (nz - 1 if way == UP else 0):
                go_if(mine, wo_loose(wox.at[zs], zs, way), ("x", way), nout - split)
            go_if(mine, wo_loose_cross(zs), ("cross", way), nout - split)

        def query_copy():
            return remote(qb.at[0], qb.at[1], pt_ss.at[0], pt_rs.at[0], below)

        def part_copies(to):
            return (
                remote(part, pin, pt_ss.at[1], pt_rs.at[1], to),
                remote(lse, lin, pt_ss.at[2], pt_rs.at[2], to),
            )

        order = (KA, KB, WQ) if top else (WQ, KA, KB)
        for item in order:
            loads[item].wait()
            if not top and (bottom or item != KB):
                own_send(item, UP)
            if top or (not bottom and item != WQ):
                own_send(item, DOWN)
            own_send(item, SIDE)
        loads[4].wait()
        go_if(t != z, wo_cross(z), ("own",), nout)

        @pl.when(t == z)
        def _():
            wo_block(t, c)[...] = woc[...]

        loads[3].wait()

        if top:
            @pl.when(c == 0)
            def _():
                kvb[:, z, rows:, :] = jnp.zeros((2, rows, HD), kvb.dtype)

        waiting = [(WQ, z), (KA, z), (KB, z)]

        def step(item, zz, *ways, keep=2):
            event(item, zz, *ways)
            waiting.append((item, zz))
            settle(keep)

        def settle(keep):
            while len(waiting) > keep:
                dot(*waiting.pop(0))

        if bottom:
            step(KA, 1)
            collect()
            loose(UP)
            hub(UP, 0, 1, 2, 3)
            step(KB, 1)
            for zz in range(2, nz):
                step(KA, zz)
                step(KB, zz)
            settle(0)
            finish_kv(KA, KB)
            for zz in range(1, nz):
                step(WQ, zz, keep=1)
            take_kv(z)
            settle(0)
            finish_q()
            need_kv(z)
            state = attend(None, 0, z)
        elif top:
            step(WQ, 2)
            step(KA, 2)
            collect()
            loose(DOWN)
            hub(DOWN, 0, 1, 2, 3)
            step(WQ, 1)
            step(KB, 2)
            step(WQ, 0)
            settle(0)
            finish_q()
            go(query_copy(), ("query",), rows)
            step(KA, 1, keep=1)
            step(KB, 1, keep=1)
            step(KA, 0, keep=1)
            step(KB, 0, keep=1)
            finish_kv(KA)
            settle(0)
            finish_kv(KB)
            take_kv(z)
            need_kv(z)
            peak, total, value = attend(None, 0, z)
            for zz in range(nz - 2, -1, -1):
                relay_loose(UP, zz)
            for copy in part_copies(below):
                copy.wait_recv()
            side = jnp.transpose(jnp.broadcast_to(lin[0:1, :], (HD, rows)))[:, 0:1]
            best = jnp.maximum(peak, side)
            near, far = jnp.exp(peak - best), jnp.exp(side - best)
            state = (
                best, total * near + far, value * near + pin[...].astype(jnp.float32) * far
            )
        elif z == 1:
            step(WQ, 0, UP)
            own_send(KB, UP)
            step(KA, 2, DOWN)
            step(KA, 0, UP)
            step(KB, 2, DOWN)
            step(KA, 3, DOWN)
            step(KB, 0, UP)
            step(KB, 3, DOWN)
            own_send(WQ, DOWN)
            collect()
            settle(0)
            finish_kv(KA, KB)
            loose(UP)
            hub(UP, 0, 1, 2, 3)
            relay(UP, 0, 1, 2, 3)
            relay_loose(UP, 0)
            step(WQ, 2, DOWN)
            step(WQ, 3, DOWN)
            loose(DOWN)
            hub(DOWN, 0, 1, 2, 3)
            take_kv(z)
            settle(0)
            finish_q()
            need_kv(z)
            state = attend(None, 0, z)
            relay(DOWN, 0, 1)
            relay_loose(DOWN, 2)
            relay_loose(DOWN, 3)
            take_kv(0)
            relay(DOWN, 2, 3)
            need_kv(0)
            state = attend(state, 0, 0)
        else:
            step(WQ, 1, UP)
            own_send(KB, UP)
            step(KA, 3, DOWN)
            step(KB, 3, DOWN)
            own_send(WQ, DOWN)
            step(KA, 1)
            step(WQ, 3, DOWN)
            step(WQ, 0, UP)
            go_chain(KA, 1, UP)
            collect()
            loose(DOWN)
            hub(DOWN, 0, 1, 2, 3)
            step(KB, 1, UP)
            relay(DOWN, 0)
            relay_loose(DOWN, 3)
            step(KA, 0, UP)
            relay(DOWN, 1)
            step(KB, 0, UP)
            loose(UP)
            hub(UP, 0)
            settle(0)
            finish_kv(KA, KB)
            finish_q()
            relay(DOWN, 2, 3)
            take_kv(1)
            need_kv(1)
            state = attend(None, 0, 1)
            query_copy().wait_recv()
            other = attend(None, 1, 1)
            take_kv(z)
            need_kv(z)
            other = attend(other, 1, z)
            state = attend(state, 0, z)
            relay(UP, 0, only=1)
            relay_loose(UP, 1)
            relay_loose(UP, 0)
            take_kv(0)
            need_kv(0)
            peak, total, value = attend(other, 1, 0)
            part[...] = (value / total).astype(jnp.bfloat16)
            lse[...] = jnp.transpose(
                jnp.broadcast_to(peak + jnp.log(total), (rows, HD))
            )[:lse.shape[0], :]
            for copy in part_copies(above):
                copy.start()
            hub(UP, 1, 2, 3)
            relay(UP, 0, only=0)
            state = attend(state, 0, 0)
            relay(UP, 1)

        hloc[...] = (state[2] / state[1]).astype(jnp.bfloat16)
        for k in range(1, nt):
            head_copy(k).start()
        head_cols(t)[...] = hloc[...]

        if bottom:
            for zz in range(1, nz):
                relay_loose(DOWN, zz)
            relay(DOWN, 0, 1, 2, 3)
        elif top:
            relay(UP, 0, 1, 2, 3)
        elif z == 2:
            relay(UP, 2, 3)

        @pl.when(t != z)
        def _():
            received(wox.at[0], wx_rs.at[nz])

        @pl.when(t < z)
        def _():
            wo_pass(last, c).start()

        @pl.when(t > z)
        def _():
            wo_pass(0, c).start()
        received(wof.at[pl.ds(pl.multiple_of((1 - c) * nout, 64), nout)], wp_rs.at[0])
        received(hid.at[:, pl.ds(0, (nt - 1) * HD)], h_rs.at[0])
        out_ref[...] = lax.dot_general(
            hcat[...], wof[...], (((1,), (1,)), ((), ())), preferred_element_type=jnp.float32
        ).astype(out_ref.dtype)
        drain(h_ss.at[0], (nt - 1) * rows)
        drain(wp_ss.at[0], nt * nout)
        end_kv()
        if z == nz - 2:
            for copy in part_copies(above):
                copy.wait_send()
        for way, ends_here, mine in ((UP, top, t <= z), (DOWN, bottom, t >= z)):
            if not ends_here:
                @pl.when(mine)
                def _():
                    drain(wc_ss.at[1, way], (nt - 1) * nout)
                    drain(wc_ss.at[0, way], split)
        for key, (amount, cond) in counts.items():
            sem = {
                "w": lambda: ss.at[key[1], key[2]], "far": lambda: kv_ss.at[0],
                "pass": lambda: kp_ss.at[0], "x": lambda: wx_ss.at[key[1]],
                "cross": lambda: wi_ss.at[1], "own": lambda: wi_ss.at[0],
                "query": lambda: pt_ss.at[0],
            }[key[0]]()
            if cond is None:
                drain(sem, amount)
            else:
                @pl.when(cond)
                def _():
                    drain(sem, amount)

    for z in range(nz):
        @pl.when(plane_of == z)
        def _():
            plane(z)


def fused_body(nz, nt, hidden_states, resp_lengths, w_query, w_keyval, w_out):
    rows, depth = hidden_states.shape
    nout = w_out.shape[1]
    bf16, f32 = jnp.bfloat16, jnp.float32
    dma = pltpu.SemaphoreType.DMA
    hbm = pl.BlockSpec(memory_space=pltpu.HBM)
    return pl.pallas_call(
        functools.partial(fused_kernel, nz, nt),
        out_shape=jax.ShapeDtypeStruct((rows, 2 * nout), bf16),
        in_specs=[hbm] * 5,
        out_specs=pl.BlockSpec(memory_space=pltpu.VMEM),
        scratch_shapes=[
            pltpu.VMEM((rows, depth), bf16),
            pltpu.VMEM((3, depth, HD), bf16),
            pltpu.VMEM((nout, HD), bf16),
            pltpu.VMEM((nz, nout * LOOSE // 8, HD), bf16),
            pltpu.VMEM((2 * nout, nt * HD), bf16),
            pltpu.VMEM((2, rows, HD), bf16),
            pltpu.VMEM((2, nz, 2 * rows, HD), bf16),
            pltpu.VMEM((3, rows, HD), f32),
            pltpu.VMEM((2, rows, HD), bf16),
            pltpu.VMEM((rows, HD), bf16),
            pltpu.VMEM((8, rows), f32),
            pltpu.VMEM((rows, HD), bf16),
            pltpu.VMEM((8, rows), f32),
            pltpu.VMEM((rows, HD), bf16),
            pltpu.VMEM((rows, nt * HD), bf16),
            dma((6,)),
            dma((2, 3)),
            dma((3, nz)),
            dma((3, nz)),
            dma((2,)),
            dma((nz,)),
            dma((1,)),
            dma((nz,)),
            dma((2, 2)),
            dma((2,)),
            dma((nz + 1,)),
            dma((2,)),
            dma((nt,)),
            dma((1,)),
            dma((1,)),
            dma((3,)),
            dma((3,)),
            dma((1,)),
            dma((1,)),
            pltpu.SMEM(resp_lengths.shape, jnp.int32),
        ],
        compiler_params=pltpu.CompilerParams(
            collective_id=0, has_side_effects=True, vmem_limit_bytes=40_000_000
        ),
    )(*[
        pltpu.with_memory_space_constraint(x, pltpu.HBM)
        for x in (resp_lengths, hidden_states, w_query, w_keyval, w_out.T)
    ])


def per_device(mesh, hidden_states, resp_lengths, w_query, w_keyval, w_out):
    nt = mesh.shape["tp"]
    nz = mesh.shape["dp"] // 2
    args = (hidden_states, resp_lengths, w_query, w_keyval, w_out)
    fits = (
        mesh.shape["dp"] == 2 * nz and nz == nt and nt == 4
        and w_query.shape[1] == HD and w_keyval.shape[1] == 2 * HD
        and w_out.shape[0] == HD and w_query.shape[0] % 64 == 0
    )
    return fused_body(nz, nt, *args) if fits else body(*args)


def solution(mesh):
    return jax.shard_map(
        functools.partial(per_device, mesh),
        mesh=mesh,
        in_specs=(P("dp", None), P(), P("dp", "tp"), P("dp", "tp"), P("tp", "dp")),
        out_specs=P("dp", "tp"),
        check_vma=False,
    )
```

```python
import functools

import jax
import jax.numpy as jnp
from jax import lax
from jax.experimental import pallas as pl
from jax.experimental.pallas import tpu as pltpu
from jax.sharding import PartitionSpec as P

HD = 128


def segment_of(position, resp_ends):
    return jnp.sum(
        (position[:, None] >= resp_ends[None, :]).astype(jnp.int32), axis=1, dtype=jnp.int32
    )


def body(hidden_states, resp_lengths, w_query, w_keyval, w_out):
    token_rows = hidden_states.shape[0]
    head_scale = HD ** (-0.5)
    pieces = (
        lax.all_gather(w_query, "dp", axis=0, tiled=True),
        lax.all_gather(w_keyval, "dp", axis=0, tiled=True),
    )
    query_sum = jnp.dot(hidden_states, pieces[0], preferred_element_type=jnp.float32)
    keyval_sum = jnp.dot(hidden_states, pieces[1], preferred_element_type=jnp.float32)
    query = (query_sum * head_scale).astype(jnp.bfloat16)
    keyval = lax.all_gather(keyval_sum.astype(jnp.bfloat16), "tp", axis=1, tiled=True)
    kv_count = keyval.shape[1] // (2 * HD)
    per_group = lax.axis_size("tp") // kv_count
    kv_head = lax.axis_index("tp") // per_group
    key_head = lax.dynamic_slice_in_dim(keyval, kv_head * HD, HD, 1)
    value_head = lax.dynamic_slice_in_dim(keyval, (kv_count + kv_head) * HD, HD, 1)
    head_pair = jnp.concatenate([key_head, value_head], axis=1)
    resp_ends = jnp.cumsum(resp_lengths, dtype=jnp.int32)
    own_begin = lax.axis_index("dp") * token_rows
    query_pos = own_begin + jnp.arange(token_rows, dtype=jnp.int32)
    query_seg = segment_of(query_pos, resp_ends)
    pieces = lax.all_gather(head_pair, "dp", axis=0, tiled=True)
    largest = jnp.full((token_rows,), -1e30, jnp.float32)
    height = pieces.shape[0]
    key_pos = jnp.arange(height, dtype=jnp.int32)
    key_seg = segment_of(key_pos, resp_ends)
    scores = jnp.dot(query, pieces[:, :HD].T, preferred_element_type=jnp.float32)
    allowed = (
        (query_seg[:, None] == key_seg[None, :])
        & (key_pos[None, :] <= query_pos[:, None])
        & (key_pos[None, :] >= 0)
    )
    newest = jnp.maximum(largest, jnp.max(jnp.where(allowed, scores, jnp.float32(-1e30)), axis=1))
    expw = jnp.where(allowed, jnp.exp(scores - newest[:, None]), jnp.float32(0.0))
    denom = jnp.sum(expw, axis=1)
    numer = jnp.dot(expw.astype(jnp.bfloat16), pieces[:, HD:], preferred_element_type=jnp.float32)
    heads_out = (numer / denom[:, None]).astype(jnp.bfloat16)
    terms = jnp.dot(
        heads_out,
        lax.all_gather(w_out, "dp", axis=1, tiled=True),
        preferred_element_type=jnp.float32,
    )
    summed = lax.psum_scatter(terms.astype(jnp.bfloat16), "tp", scatter_dimension=1, tiled=True)
    return summed


MESH = pl.DeviceIdType.MESH
KA, KB, WQ = range(3)
UP, DOWN, SIDE = range(3)
NEG = -1e30
LOOSE = ((28, 28, 12, 0), (0, 12, 24, 18))


def fused_kernel(
    nz, nt, lens_hbm, hid_hbm, wq_hbm, wkv_hbm, wo_hbm, out_ref,
    hid, w, woc, wox, wof, kvloc, kvb, acc, qb, part, lse, pin, lin, hloc, hcat,
    loc_sem, ss, rs, prs, kv_ss, kv_rs, kp_ss, kp_rs, wc_ss, wx_ss, wx_rs, wi_ss, wi_rs, wp_ss, wp_rs,
    pt_ss, pt_rs, h_ss, h_rs, lens_ref,
):
    dp = lax.axis_index("dp")
    t = lax.axis_index("tp")
    plane_of, c = dp // 2, dp % 2
    rows = hid.shape[0]
    shard = wq_hbm.shape[0]
    nout = wo_hbm.shape[0]
    own = pl.ds(pl.multiple_of(dp * shard, 64), shard)

    barrier = pltpu.get_barrier_semaphore()
    partner = {"dp": dp + 1 - 2 * c, "tp": t}
    above, below = {"dp": dp + 2, "tp": t}, {"dp": dp - 2, "tp": t}
    has_up, has_down = plane_of < nz - 1, plane_of > 0
    pl.semaphore_signal(barrier, 1, device_id=partner, device_id_type=MESH)

    @pl.when(has_up)
    def _():
        pl.semaphore_signal(barrier, 1, device_id=above, device_id_type=MESH)

    @pl.when(has_down)
    def _():
        pl.semaphore_signal(barrier, 1, device_id=below, device_id_type=MESH)

    for k in range(1, nt):
        pl.semaphore_signal(
            barrier, 1, device_id={"dp": dp, "tp": (t + k) % nt}, device_id_type=MESH
        )
    loads = [
        pltpu.make_async_copy(wkv_hbm.at[:, pl.ds(0, HD)], w.at[KA, own], loc_sem.at[KA]),
        pltpu.make_async_copy(wkv_hbm.at[:, pl.ds(HD, HD)], w.at[KB, own], loc_sem.at[KB]),
        pltpu.make_async_copy(wq_hbm, w.at[WQ, own], loc_sem.at[WQ]),
        pltpu.make_async_copy(hid_hbm, hid, loc_sem.at[3]),
        pltpu.make_async_copy(wo_hbm, woc, loc_sem.at[4]),
        pltpu.make_async_copy(lens_hbm, lens_ref, loc_sem.at[5]),
    ]
    for load in loads:
        load.start()

    pl.semaphore_wait(barrier, nt + has_up.astype(jnp.int32) + has_down.astype(jnp.int32))

    def chunk(item, zz, cc):
        return w.at[item, pl.ds(pl.multiple_of((2 * zz + cc) * shard, 64), shard)]

    def remote(src, dst, send, recv, to):
        return pltpu.make_async_remote_copy(
            src, dst, send, recv, device_id=to, device_id_type=MESH
        )

    def chain(item, zz, way):
        ref = chunk(item, zz, c)
        recv = prs.at[item, zz] if way == SIDE else rs.at[item, zz]
        return remote(
            ref, ref, ss.at[int(item == WQ), way], recv, (above, below, partner)[way]
        )

    def device(zz, tt):
        return {"dp": 2 * zz + c, "tp": tt}

    half_rows = pl.ds(pl.multiple_of(c * rows, 128), rows)
    other_rows = pl.ds(pl.multiple_of((1 - c) * rows, 128), rows)

    def kv_copy(z, b, zz):
        role = t // (nt // 2)
        return remote(
            kvloc.at[b], kvb.at[role, z, half_rows], kv_ss.at[int(zz == z)], kv_rs.at[z],
            device(zz, 2 * (t % (nt // 2)) + b),
        )

    def kv_over(z, b):
        role = t // (nt // 2)
        return remote(
            kvloc.at[b], kvb.at[role, z, pl.ds(0, rows)], kp_ss.at[0], kp_rs.at[z],
            {"dp": dp + 1, "tp": 2 * (t % (nt // 2)) + b},
        )

    def kv_pass(z, role):
        ref = kvb.at[role, z, half_rows]
        return remote(ref, ref, kp_ss.at[0], kp_rs.at[z], partner)

    def wo_block(g, cc):
        return wof.at[
            pl.ds(pl.multiple_of(cc * nout, 64), nout), pl.ds(pl.multiple_of(g * HD, HD), HD)
        ]

    def loose_rows(zs, way):
        return nout * LOOSE[way][zs] // 512 * 16

    def wo_half(g, h, zs, way):
        split = nout - loose_rows(zs, way)
        start = pl.multiple_of(c * nout + h * split, 16)
        size = nout - split if h else split
        return wof.at[pl.ds(start, size), pl.ds(pl.multiple_of(g * HD, HD), HD)]

    def loose_block(way):
        return nt - 1 if way == UP else 0

    def wo_chain(g, way, zs):
        full = int(g != loose_block(way))
        ref = wo_block(g, c) if full else wo_half(g, 0, zs, way)
        return remote(ref, ref, wc_ss.at[full, way], wi_rs.at[g], (above, below)[way])

    def wo_twin(way, zs):
        ref = wo_half(loose_block(way), 0, zs, way)
        to = {"dp": dp + (2 if way == UP else -2) + 1 - 2 * c, "tp": t}
        return remote(ref, ref, wc_ss.at[0, way], wp_rs.at[0], to)

    def wo_loose(src, zz, way):
        return remote(
            src, wox.at[zz, pl.ds(0, loose_rows(zz, way))], wx_ss.at[way], wx_rs.at[zz],
            (above, below)[way],
        )

    def wo_cross(zz):
        return remote(woc, wo_block(t, c), wi_ss.at[0], wi_rs.at[t], {"dp": dp, "tp": zz})

    def wo_loose_cross(zz, way):
        return remote(
            wox.at[zz, pl.ds(0, loose_rows(zz, way))], wo_half(t, 1, zz, way), wi_ss.at[1],
            wx_rs.at[nz], {"dp": dp, "tp": zz},
        )

    def wo_pass(g, cc):
        ref = wo_block(g, cc)
        return remote(ref, ref, wp_ss.at[0], wp_rs.at[0], partner)

    def head_cols(g):
        return hcat.at[:, pl.ds(pl.multiple_of(g * HD, HD), HD)]

    def head_copy(k):
        return remote(
            hloc, head_cols(t), h_ss.at[0], h_rs.at[0], {"dp": dp, "tp": (t + k) % nt}
        )

    loads[5].wait()
    ends = []
    end = jnp.int32(0)
    for r in range(lens_ref.shape[0]):
        end = end + lens_ref[r]
        ends.append(end)

    def plane(z):
        counts = {}
        seen = set()
        top, bottom = z == nz - 1, z == 0
        kv_to = [zz for zz in (nz - 2, nz - 3, 0) if zz >= z] if not top else [z]
        span = 2 * shard

        def tally(key, rows_sent, cond=None):
            counts[key] = (counts.get(key, (0, cond))[0] + rows_sent, cond)

        def go(copy, key, rows_sent):
            copy.start()
            tally(key, rows_sent)

        def go_chain(item, zz, way):
            go(chain(item, zz, way), ("w", int(item == WQ), way), shard)

        def received(ref, sem):
            remote(ref, ref, sem, sem, partner).wait_recv()

        def drain(sem, amount):
            ref = w.at[0, pl.ds(0, amount)]
            remote(ref, ref, sem, sem, partner).wait_send()

        def own_send(item, way):
            go_chain(item, z, way)

        def event(item, zz, *ways):
            ref = chunk(item, zz, c)
            received(ref, rs.at[item, zz])
            for way in ways + (SIDE,):
                go_chain(item, zz, way)

        def dot(item, zz):
            ref = chunk(item, zz, 1 - c)
            received(ref, prs.at[item, zz])
            part_sum = jnp.dot(
                hid[:, zz * span:(zz + 1) * span], w[item, zz * span:(zz + 1) * span, :],
                preferred_element_type=jnp.float32,
            )
            if item in seen:
                acc[item] += part_sum
            else:
                seen.add(item)
                acc[item] = part_sum

        def finish_kv(*picks):
            role = t // (nt // 2)
            for b in picks:
                kvloc[b] = acc[b].astype(jnp.bfloat16)
            for zz in kv_to:
                if zz != z:
                    for b in picks:
                        go(kv_copy(z, b, zz), ("far",), rows)
            for b in picks:
                mine = 2 * (t % (nt // 2)) + b == t
                if top:
                    go_if(c == 0, kv_over(z, b), ("pass",), rows)

                @pl.when(jnp.logical_not(mine))
                def _():
                    kv_copy(z, b, z).start()

                @pl.when(mine)
                def _():
                    kvb[role, z, half_rows, :] = kvloc[b]

        k_here, v_here = t // 2 == t, t // 2 + nt // 2 == t
        none_here = jnp.logical_not(jnp.logical_or(k_here, v_here))

        def end_kv():
            @pl.when(none_here)
            def _():
                drain(kv_ss.at[1], 2 * rows)

            @pl.when(jnp.logical_not(none_here))
            def _():
                drain(kv_ss.at[1], rows)

        def take_kv(zs):
            both = kvb.at[:, zs, half_rows]
            if zs == z:
                @pl.when(none_here)
                def _():
                    received(both, kv_rs.at[zs])

                @pl.when(jnp.logical_not(none_here))
                def _():
                    received(kvb.at[jnp.where(k_here, 1, 0), zs, half_rows], kv_rs.at[zs])
            else:
                received(both, kv_rs.at[zs])
            if not top:
                for role in range(2):
                    go(kv_pass(zs, role), ("pass",), rows)

        def need_kv(zs):
            both = kvb.at[:, zs, other_rows]
            if top:
                @pl.when(c == 1)
                def _():
                    received(both, kp_rs.at[zs])
            else:
                received(both, kp_rs.at[zs])

        def finish_q():
            qb[0] = (acc[WQ] * (HD ** -0.5)).astype(jnp.bfloat16)

        def attend(state, qi, zs):
            qpos = (dp + 2 * qi) * rows + lax.broadcasted_iota(jnp.int32, (rows, 1), 0)
            first = jnp.zeros((rows, 1), jnp.int32)
            for e in ends:
                first = jnp.where(qpos >= e, e, first)
            s = lax.dot_general(
                qb[qi], kvb[0, zs], (((1,), (1,)), ((), ())), preferred_element_type=jnp.float32
            )
            kpos = zs * 2 * rows + lax.broadcasted_iota(jnp.int32, s.shape, 1)
            s = jnp.where((kpos >= first) & (kpos <= qpos), s, jnp.float32(NEG))
            peak = jnp.max(s, axis=1, keepdims=True)
            if state is not None:
                peak = jnp.maximum(state[0], peak)
            p = jnp.exp(s - peak)
            total = jnp.sum(p, axis=1, keepdims=True)
            value = jnp.dot(
                p.astype(jnp.bfloat16), kvb[1, zs], preferred_element_type=jnp.float32
            )
            if state is not None:
                fade = jnp.exp(state[0] - peak)
                total = total + state[1] * fade
                value = value + state[2] * fade
            return peak, total, value

        last = nt - 1

        def go_if(cond, copy, key, rows_sent):
            @pl.when(cond)
            def _():
                copy.start()
            tally(key, rows_sent, cond)

        def wo_arrived(g, ref):
            received(ref, wi_rs.at[g])

        def collect():
            @pl.when(t == z)
            def _():
                for g in range(nt):
                    if g != z:
                        wo_arrived(g, wo_block(g, c))
                    wo_pass(g, c).start()

        def last_hop(way):
            return z == (nz - 2 if way == UP else 1)

        def send_on(g, way, zs):
            wo_chain(g, way, zs).start()
            if g == loose_block(way) and last_hop(way):
                wo_twin(way, zs).start()

        def hub(way, *picks):
            for k in picks:
                @pl.when(t == z)
                def _():
                    send_on(k if way == UP else (k + 1) % nt, way, z)

        def loose(way):
            size = loose_rows(z, way)
            go_if(
                t == (last if way == UP else 0),
                wo_loose(woc.at[pl.ds(nout - size, size)], z, way), ("x", way), size,
            )

        def relay(way, *picks, only=None):
            if z == (0 if way == UP else nz - 1):
                return
            ends = z == (nz - 1 if way == UP else 0)
            mine = t < z if way == UP else t > z
            if only is not None:
                mine = t == only
            for k in picks:
                g = k if way == UP else (k + 1) % nt
                if k < nt - 1:
                    @pl.when(mine)
                    def _():
                        wo_arrived(g, wo_block(g, c))
                        if not ends:
                            send_on(g, way, None)
                        wo_pass(g, c).start()
                else:
                    for zs in range(z) if way == UP else range(z + 1, nz):
                        @pl.when(t == zs)
                        def _():
                            wo_arrived(g, wo_half(g, 0, zs, way))
                            if not ends:
                                send_on(g, way, zs)

        def relay_loose(way, zs):
            mine = t == (last if way == UP else 0)
            size = loose_rows(zs, way)

            @pl.when(mine)
            def _():
                received(wox.at[zs, pl.ds(0, size)], wx_rs.at[zs])
            if z != (nz - 1 if way == UP else 0):
                go_if(
                    mine, wo_loose(wox.at[zs, pl.ds(0, size)], zs, way), ("x", way), size
                )
            go_if(mine, wo_loose_cross(zs, way), ("cross", way), size)

        def query_copy():
            return remote(qb.at[0], qb.at[1], pt_ss.at[0], pt_rs.at[0], below)

        def part_copies(to):
            return (
                remote(part, pin, pt_ss.at[1], pt_rs.at[1], to),
                remote(lse, lin, pt_ss.at[2], pt_rs.at[2], to),
            )

        order = (KA, KB, WQ) if top else (WQ, KA, KB)
        for item in order:
            loads[item].wait()
            if not top and (bottom or item != KB):
                own_send(item, UP)
            if top or (not bottom and item != WQ):
                own_send(item, DOWN)
            own_send(item, SIDE)
        loads[4].wait()
        go_if(t != z, wo_cross(z), ("own",), nout)

        @pl.when(t == z)
        def _():
            wo_block(t, c)[...] = woc[...]

        loads[3].wait()

        if top:
            @pl.when(c == 0)
            def _():
                kvb[:, z, rows:, :] = jnp.zeros((2, rows, HD), kvb.dtype)

        waiting = [(WQ, z), (KA, z), (KB, z)]

        def step(item, zz, *ways, keep=2):
            event(item, zz, *ways)
            waiting.append((item, zz))
            settle(keep)

        def settle(keep):
            while len(waiting) > keep:
                dot(*waiting.pop(0))

        if bottom:
            step(KA, 1)
            collect()
            loose(UP)
            hub(UP, 0, 1, 2, 3)
            step(KB, 1)
            for zz in range(2, nz):
                step(KA, zz)
                step(KB, zz)
            settle(0)
            finish_kv(KA, KB)
            for zz in range(1, nz):
                step(WQ, zz, keep=1)
            take_kv(z)
            settle(0)
            finish_q()
            need_kv(z)
            state = attend(None, 0, z)
        elif top:
            step(WQ, 2)
            step(KA, 2)
            collect()
            loose(DOWN)
            hub(DOWN, 0, 1, 2, 3)
            step(WQ, 1)
            step(KB, 2)
            step(WQ, 0)
            settle(0)
            finish_q()
            go(query_copy(), ("query",), rows)
            step(KA, 1, keep=1)
            step(KB, 1, keep=1)
            step(KA, 0, keep=1)
            step(KB, 0, keep=1)
            finish_kv(KA)
            settle(0)
            finish_kv(KB)
            take_kv(z)
            need_kv(z)
            peak, total, value = attend(None, 0, z)
            for zz in range(nz - 2, -1, -1):
                relay_loose(UP, zz)
            for copy in part_copies(below):
                copy.wait_recv()
            side = jnp.transpose(jnp.broadcast_to(lin[0:1, :], (HD, rows)))[:, 0:1]
            best = jnp.maximum(peak, side)
            near, far = jnp.exp(peak - best), jnp.exp(side - best)
            state = (
                best, total * near + far, value * near + pin[...].astype(jnp.float32) * far
            )
        elif z == 1:
            step(WQ, 0, UP)
            own_send(KB, UP)
            step(KA, 2, DOWN)
            step(KA, 0, UP)
            step(KB, 2, DOWN)
            step(KA, 3, DOWN)
            step(KB, 0, UP)
            step(KB, 3, DOWN)
            own_send(WQ, DOWN)
            collect()
            settle(0)
            finish_kv(KA, KB)
            loose(UP)
            hub(UP, 0, 1, 2, 3)
            relay(UP, 0, 1, 2, 3)
            relay_loose(UP, 0)
            step(WQ, 2, DOWN)
            step(WQ, 3, DOWN)
            loose(DOWN)
            hub(DOWN, 0, 1, 2, 3)
            take_kv(z)
            settle(0)
            finish_q()
            need_kv(z)
            state = attend(None, 0, z)
            relay(DOWN, 0, 1)
            relay_loose(DOWN, 2)
            relay_loose(DOWN, 3)
            take_kv(0)
            relay(DOWN, 2, 3)
            need_kv(0)
            state = attend(state, 0, 0)
        else:
            step(WQ, 1, UP)
            own_send(KB, UP)
            step(KA, 3, DOWN)
            step(KB, 3, DOWN)
            own_send(WQ, DOWN)
            step(KA, 1)
            step(WQ, 3, DOWN)
            step(WQ, 0, UP)
            go_chain(KA, 1, UP)
            collect()
            loose(DOWN)
            hub(DOWN, 0, 1, 2, 3)
            step(KB, 1, UP)
            relay(DOWN, 0)
            relay_loose(DOWN, 3)
            step(KA, 0, UP)
            relay(DOWN, 1)
            step(KB, 0, UP)
            loose(UP)
            hub(UP, 0)
            settle(0)
            finish_kv(KA, KB)
            finish_q()
            relay(DOWN, 2, 3)
            take_kv(1)
            need_kv(1)
            state = attend(None, 0, 1)
            query_copy().wait_recv()
            other = attend(None, 1, 1)
            take_kv(z)
            need_kv(z)
            other = attend(other, 1, z)
            state = attend(state, 0, z)
            relay(UP, 0, only=1)
            relay_loose(UP, 1)
            relay_loose(UP, 0)
            take_kv(0)
            need_kv(0)
            peak, total, value = attend(other, 1, 0)
            part[...] = (value / total).astype(jnp.bfloat16)
            lse[...] = jnp.transpose(
                jnp.broadcast_to(peak + jnp.log(total), (rows, HD))
            )[:lse.shape[0], :]
            for copy in part_copies(above):
                copy.start()
            hub(UP, 1, 2, 3)
            relay(UP, 0, only=0)
            state = attend(state, 0, 0)
            relay(UP, 1)

        hloc[...] = (state[2] / state[1]).astype(jnp.bfloat16)
        for k in range(1, nt):
            head_copy(k).start()
        head_cols(t)[...] = hloc[...]

        if bottom:
            for zz in range(1, nz):
                relay_loose(DOWN, zz)
            relay(DOWN, 0, 1, 2, 3)
        elif top:
            relay(UP, 0, 1, 2, 3)
        elif z == 2:
            relay(UP, 2, 3)

        for zs in range(nz):
            if zs != z:
                way = UP if zs < z else DOWN
                g = loose_block(way)

                @pl.when(t == zs)
                def _():
                    late = wo_half(g, 1, zs, way)
                    received(late, wx_rs.at[nz])
                    if top or bottom:
                        remote(late, late, wp_ss.at[0], wp_rs.at[0], partner).start()
                    else:
                        wo_pass(g, c).start()
        received(wof.at[pl.ds(pl.multiple_of((1 - c) * nout, 64), nout)], wp_rs.at[0])
        received(hid.at[:, pl.ds(0, (nt - 1) * HD)], h_rs.at[0])
        out_ref[...] = lax.dot_general(
            hcat[...], wof[...], (((1,), (1,)), ((), ())), preferred_element_type=jnp.float32
        ).astype(out_ref.dtype)
        drain(h_ss.at[0], (nt - 1) * rows)
        drain(wp_ss.at[0], (nt - 1) * nout)
        for zs in range(nz):
            way = UP if zs < z else DOWN
            part_only = zs != z and (top or bottom)

            @pl.when(t == zs)
            def _():
                drain(wp_ss.at[0], loose_rows(zs, way) if part_only else nout)
        end_kv()
        if z == nz - 2:
            for copy in part_copies(above):
                copy.wait_send()
        for way, ends_here, mine in ((UP, top, t <= z), (DOWN, bottom, t >= z)):
            if not ends_here:
                @pl.when(mine)
                def _():
                    drain(wc_ss.at[1, way], (nt - 1) * nout)
                for zs in range(z + 1) if way == UP else range(z, nz):
                    @pl.when(t == zs)
                    def _():
                        rest = nout - loose_rows(zs, way)
                        drain(wc_ss.at[0, way], rest * (2 if last_hop(way) else 1))
        for key, (amount, cond) in counts.items():
            sem = {
                "w": lambda: ss.at[key[1], key[2]], "far": lambda: kv_ss.at[0],
                "pass": lambda: kp_ss.at[0], "x": lambda: wx_ss.at[key[1]],
                "cross": lambda: wi_ss.at[1], "own": lambda: wi_ss.at[0],
                "query": lambda: pt_ss.at[0],
            }[key[0]]()
            if cond is None:
                drain(sem, amount)
            else:
                @pl.when(cond)
                def _():
                    drain(sem, amount)

    for z in range(nz):
        @pl.when(plane_of == z)
        def _():
            plane(z)


def fused_body(nz, nt, hidden_states, resp_lengths, w_query, w_keyval, w_out):
    rows, depth = hidden_states.shape
    nout = w_out.shape[1]
    bf16, f32 = jnp.bfloat16, jnp.float32
    dma = pltpu.SemaphoreType.DMA
    hbm = pl.BlockSpec(memory_space=pltpu.HBM)
    return pl.pallas_call(
        functools.partial(fused_kernel, nz, nt),
        out_shape=jax.ShapeDtypeStruct((rows, 2 * nout), bf16),
        in_specs=[hbm] * 5,
        out_specs=pl.BlockSpec(memory_space=pltpu.VMEM),
        scratch_shapes=[
            pltpu.VMEM((rows, depth), bf16),
            pltpu.VMEM((3, depth, HD), bf16),
            pltpu.VMEM((nout, HD), bf16),
            pltpu.VMEM((nz, nout, HD), bf16),
            pltpu.VMEM((2 * nout, nt * HD), bf16),
            pltpu.VMEM((2, rows, HD), bf16),
            pltpu.VMEM((2, nz, 2 * rows, HD), bf16),
            pltpu.VMEM((3, rows, HD), f32),
            pltpu.VMEM((2, rows, HD), bf16),
            pltpu.VMEM((rows, HD), bf16),
            pltpu.VMEM((8, rows), f32),
            pltpu.VMEM((rows, HD), bf16),
            pltpu.VMEM((8, rows), f32),
            pltpu.VMEM((rows, HD), bf16),
            pltpu.VMEM((rows, nt * HD), bf16),
            dma((6,)),
            dma((2, 3)),
            dma((3, nz)),
            dma((3, nz)),
            dma((2,)),
            dma((nz,)),
            dma((1,)),
            dma((nz,)),
            dma((2, 2)),
            dma((2,)),
            dma((nz + 1,)),
            dma((2,)),
            dma((nt,)),
            dma((1,)),
            dma((1,)),
            dma((3,)),
            dma((3,)),
            dma((1,)),
            dma((1,)),
            pltpu.SMEM(resp_lengths.shape, jnp.int32),
        ],
        compiler_params=pltpu.CompilerParams(
            collective_id=0, has_side_effects=True, vmem_limit_bytes=40_000_000
        ),
    )(*[
        pltpu.with_memory_space_constraint(x, pltpu.HBM)
        for x in (resp_lengths, hidden_states, w_query, w_keyval, w_out.T)
    ])


def per_device(mesh, hidden_states, resp_lengths, w_query, w_keyval, w_out):
    nt = mesh.shape["tp"]
    nz = mesh.shape["dp"] // 2
    args = (hidden_states, resp_lengths, w_query, w_keyval, w_out)
    fits = (
        mesh.shape["dp"] == 2 * nz and nz == nt and nt == 4
        and w_query.shape[1] == HD and w_keyval.shape[1] == 2 * HD
        and w_out.shape[0] == HD and w_query.shape[0] % 64 == 0
    )
    return fused_body(nz, nt, *args) if fits else body(*args)


def solution(mesh):
    return jax.shard_map(
        functools.partial(per_device, mesh),
        mesh=mesh,
        in_specs=(P("dp", None), P(), P("dp", "tp"), P("dp", "tp"), P("tp", "dp")),
        out_specs=P("dp", "tp"),
        check_vma=False,
    )
```

```python
import functools

import jax
import jax.numpy as jnp
from jax import lax
from jax.experimental import pallas as pl
from jax.experimental.pallas import tpu as pltpu
from jax.sharding import PartitionSpec as P

HD = 128


def segment_of(position, resp_ends):
    return jnp.sum(
        (position[:, None] >= resp_ends[None, :]).astype(jnp.int32), axis=1, dtype=jnp.int32
    )


def body(hidden_states, resp_lengths, w_query, w_keyval, w_out):
    token_rows = hidden_states.shape[0]
    head_scale = HD ** (-0.5)
    pieces = (
        lax.all_gather(w_query, "dp", axis=0, tiled=True),
        lax.all_gather(w_keyval, "dp", axis=0, tiled=True),
    )
    query_sum = jnp.dot(hidden_states, pieces[0], preferred_element_type=jnp.float32)
    keyval_sum = jnp.dot(hidden_states, pieces[1], preferred_element_type=jnp.float32)
    query = (query_sum * head_scale).astype(jnp.bfloat16)
    keyval = lax.all_gather(keyval_sum.astype(jnp.bfloat16), "tp", axis=1, tiled=True)
    kv_count = keyval.shape[1] // (2 * HD)
    per_group = lax.axis_size("tp") // kv_count
    kv_head = lax.axis_index("tp") // per_group
    key_head = lax.dynamic_slice_in_dim(keyval, kv_head * HD, HD, 1)
    value_head = lax.dynamic_slice_in_dim(keyval, (kv_count + kv_head) * HD, HD, 1)
    head_pair = jnp.concatenate([key_head, value_head], axis=1)
    resp_ends = jnp.cumsum(resp_lengths, dtype=jnp.int32)
    own_begin = lax.axis_index("dp") * token_rows
    query_pos = own_begin + jnp.arange(token_rows, dtype=jnp.int32)
    query_seg = segment_of(query_pos, resp_ends)
    pieces = lax.all_gather(head_pair, "dp", axis=0, tiled=True)
    largest = jnp.full((token_rows,), -1e30, jnp.float32)
    height = pieces.shape[0]
    key_pos = jnp.arange(height, dtype=jnp.int32)
    key_seg = segment_of(key_pos, resp_ends)
    scores = jnp.dot(query, pieces[:, :HD].T, preferred_element_type=jnp.float32)
    allowed = (
        (query_seg[:, None] == key_seg[None, :])
        & (key_pos[None, :] <= query_pos[:, None])
        & (key_pos[None, :] >= 0)
    )
    newest = jnp.maximum(largest, jnp.max(jnp.where(allowed, scores, jnp.float32(-1e30)), axis=1))
    expw = jnp.where(allowed, jnp.exp(scores - newest[:, None]), jnp.float32(0.0))
    denom = jnp.sum(expw, axis=1)
    numer = jnp.dot(expw.astype(jnp.bfloat16), pieces[:, HD:], preferred_element_type=jnp.float32)
    heads_out = (numer / denom[:, None]).astype(jnp.bfloat16)
    terms = jnp.dot(
        heads_out,
        lax.all_gather(w_out, "dp", axis=1, tiled=True),
        preferred_element_type=jnp.float32,
    )
    summed = lax.psum_scatter(terms.astype(jnp.bfloat16), "tp", scatter_dimension=1, tiled=True)
    return summed


MESH = pl.DeviceIdType.MESH
KA, KB, WQ = range(3)
UP, DOWN, SIDE = range(3)
NEG = -1e30
LOOSE = ((28, 28, 12, 0), (0, 12, 24, 18))


def fused_kernel(
    nz, nt, lens_hbm, hid_hbm, wq_hbm, wkv_hbm, wo_hbm, out_ref,
    hid, w, woc, wox, wof, kvloc, kvb, acc, qb, part, lse, pin, lin, hloc, hcat,
    loc_sem, ss, rs, prs, kv_ss, kv_rs, kp_ss, kp_rs, wc_ss, wx_ss, wx_rs, wi_ss, wi_rs, wp_ss, wp_rs,
    pt_ss, pt_rs, h_ss, h_rs, lens_ref,
):
    dp = lax.axis_index("dp")
    t = lax.axis_index("tp")
    plane_of, c = dp // 2, dp % 2
    rows = hid.shape[0]
    shard = wq_hbm.shape[0]
    nout = wo_hbm.shape[0]
    own = pl.ds(pl.multiple_of(dp * shard, 64), shard)

    barrier = pltpu.get_barrier_semaphore()
    partner = {"dp": dp + 1 - 2 * c, "tp": t}
    above, below = {"dp": dp + 2, "tp": t}, {"dp": dp - 2, "tp": t}
    has_up, has_down = plane_of < nz - 1, plane_of > 0
    pl.semaphore_signal(barrier, 1, device_id=partner, device_id_type=MESH)

    @pl.when(has_up)
    def _():
        pl.semaphore_signal(barrier, 1, device_id=above, device_id_type=MESH)

    @pl.when(has_down)
    def _():
        pl.semaphore_signal(barrier, 1, device_id=below, device_id_type=MESH)

    for k in range(1, nt):
        pl.semaphore_signal(
            barrier, 1, device_id={"dp": dp, "tp": (t + k) % nt}, device_id_type=MESH
        )
    loads = [
        pltpu.make_async_copy(wkv_hbm.at[:, pl.ds(0, HD)], w.at[KA, own], loc_sem.at[KA]),
        pltpu.make_async_copy(wkv_hbm.at[:, pl.ds(HD, HD)], w.at[KB, own], loc_sem.at[KB]),
        pltpu.make_async_copy(wq_hbm, w.at[WQ, own], loc_sem.at[WQ]),
        pltpu.make_async_copy(hid_hbm, hid, loc_sem.at[3]),
        pltpu.make_async_copy(wo_hbm, woc, loc_sem.at[4]),
        pltpu.make_async_copy(lens_hbm, lens_ref, loc_sem.at[5]),
    ]
    for load in loads:
        load.start()

    pl.semaphore_wait(barrier, nt + has_up.astype(jnp.int32) + has_down.astype(jnp.int32))

    def chunk(item, zz, cc):
        return w.at[item, pl.ds(pl.multiple_of((2 * zz + cc) * shard, 64), shard)]

    def remote(src, dst, send, recv, to):
        return pltpu.make_async_remote_copy(
            src, dst, send, recv, device_id=to, device_id_type=MESH
        )

    def chain(item, zz, way):
        ref = chunk(item, zz, c)
        recv = prs.at[item, zz] if way == SIDE else rs.at[item, zz]
        return remote(
            ref, ref, ss.at[int(item == WQ), way], recv, (above, below, partner)[way]
        )

    def device(zz, tt):
        return {"dp": 2 * zz + c, "tp": tt}

    half_rows = pl.ds(pl.multiple_of(c * rows, 128), rows)
    other_rows = pl.ds(pl.multiple_of((1 - c) * rows, 128), rows)

    def kv_copy(z, b, zz):
        role = t // (nt // 2)
        return remote(
            kvloc.at[b], kvb.at[role, z, half_rows], kv_ss.at[int(zz == z)], kv_rs.at[z],
            device(zz, 2 * (t % (nt // 2)) + b),
        )

    def kv_over(z, b):
        role = t // (nt // 2)
        return remote(
            kvloc.at[b], kvb.at[role, z, pl.ds(0, rows)], kp_ss.at[0], kp_rs.at[z],
            {"dp": dp + 1, "tp": 2 * (t % (nt // 2)) + b},
        )

    def kv_pass(z, role):
        ref = kvb.at[role, z, half_rows]
        return remote(ref, ref, kp_ss.at[0], kp_rs.at[z], partner)

    def wo_block(g, cc):
        return wof.at[
            pl.ds(pl.multiple_of(cc * nout, 64), nout), pl.ds(pl.multiple_of(g * HD, HD), HD)
        ]

    def loose_rows(zs, way):
        return nout * LOOSE[way][zs] // 512 * 16

    def wo_half(g, h, zs, way):
        split = nout - loose_rows(zs, way)
        start = pl.multiple_of(c * nout + h * split, 16)
        size = nout - split if h else split
        return wof.at[pl.ds(start, size), pl.ds(pl.multiple_of(g * HD, HD), HD)]

    def loose_block(way):
        return nt - 1 if way == UP else 0

    def wo_piece(g, h):
        start = pl.multiple_of(c * nout + h * (nout // 2), 16)
        return wof.at[pl.ds(start, nout // 2), pl.ds(pl.multiple_of(g * HD, HD), HD)]

    def wo_chain(g, way, zs, h=0):
        full = int(g != loose_block(way))
        ref = wo_piece(g, h) if full else wo_half(g, 0, zs, way)
        return remote(ref, ref, wc_ss.at[full, way], wi_rs.at[g, h], (above, below)[way])

    def wo_twin(way, zs):
        ref = wo_half(loose_block(way), 0, zs, way)
        to = {"dp": dp + (2 if way == UP else -2) + 1 - 2 * c, "tp": t}
        return remote(ref, ref, wc_ss.at[0, way], wp_rs.at[0], to)

    def wo_loose(src, zz, way):
        return remote(
            src, wox.at[zz, pl.ds(0, loose_rows(zz, way))], wx_ss.at[way], wx_rs.at[zz],
            (above, below)[way],
        )

    def wo_cross(zz):
        return remote(woc, wo_block(t, c), wi_ss.at[0], wi_rs.at[t, 0], {"dp": dp, "tp": zz})

    def wo_loose_cross(zz, way):
        return remote(
            wox.at[zz, pl.ds(0, loose_rows(zz, way))], wo_half(t, 1, zz, way), wi_ss.at[1],
            wx_rs.at[nz], {"dp": dp, "tp": zz},
        )

    def wo_pass(g, cc):
        ref = wo_block(g, cc)
        return remote(ref, ref, wp_ss.at[0], wp_rs.at[0], partner)

    def head_cols(g):
        return hcat.at[:, pl.ds(pl.multiple_of(g * HD, HD), HD)]

    def head_copy(k):
        return remote(
            hloc, head_cols(t), h_ss.at[0], h_rs.at[0], {"dp": dp, "tp": (t + k) % nt}
        )

    loads[5].wait()
    ends = []
    end = jnp.int32(0)
    for r in range(lens_ref.shape[0]):
        end = end + lens_ref[r]
        ends.append(end)

    def plane(z):
        counts = {}
        seen = set()
        top, bottom = z == nz - 1, z == 0
        kv_to = [zz for zz in (nz - 2, nz - 3, 0) if zz >= z] if not top else [z]
        span = 2 * shard

        def tally(key, rows_sent, cond=None):
            counts[key] = (counts.get(key, (0, cond))[0] + rows_sent, cond)

        def go(copy, key, rows_sent):
            copy.start()
            tally(key, rows_sent)

        def go_chain(item, zz, way):
            go(chain(item, zz, way), ("w", int(item == WQ), way), shard)

        def received(ref, sem):
            remote(ref, ref, sem, sem, partner).wait_recv()

        def drain(sem, amount):
            ref = w.at[0, pl.ds(0, amount)]
            remote(ref, ref, sem, sem, partner).wait_send()

        def own_send(item, way):
            go_chain(item, z, way)

        def event(item, zz, *ways):
            ref = chunk(item, zz, c)
            received(ref, rs.at[item, zz])
            for way in ways + (SIDE,):
                go_chain(item, zz, way)

        def dot(item, zz):
            ref = chunk(item, zz, 1 - c)
            received(ref, prs.at[item, zz])
            part_sum = jnp.dot(
                hid[:, zz * span:(zz + 1) * span], w[item, zz * span:(zz + 1) * span, :],
                preferred_element_type=jnp.float32,
            )
            if item in seen:
                acc[item] += part_sum
            else:
                seen.add(item)
                acc[item] = part_sum

        def finish_kv(*picks):
            role = t // (nt // 2)
            for b in picks:
                kvloc[b] = acc[b].astype(jnp.bfloat16)
            for zz in kv_to:
                if zz != z:
                    for b in picks:
                        go(kv_copy(z, b, zz), ("far",), rows)
            for b in picks:
                mine = 2 * (t % (nt // 2)) + b == t
                if top:
                    go_if(c == 0, kv_over(z, b), ("pass",), rows)

                @pl.when(jnp.logical_not(mine))
                def _():
                    kv_copy(z, b, z).start()

                @pl.when(mine)
                def _():
                    kvb[role, z, half_rows, :] = kvloc[b]

        k_here, v_here = t // 2 == t, t // 2 + nt // 2 == t
        none_here = jnp.logical_not(jnp.logical_or(k_here, v_here))

        def end_kv():
            @pl.when(none_here)
            def _():
                drain(kv_ss.at[1], 2 * rows)

            @pl.when(jnp.logical_not(none_here))
            def _():
                drain(kv_ss.at[1], rows)

        def take_kv(zs):
            both = kvb.at[:, zs, half_rows]
            if zs == z:
                @pl.when(none_here)
                def _():
                    received(both, kv_rs.at[zs])

                @pl.when(jnp.logical_not(none_here))
                def _():
                    received(kvb.at[jnp.where(k_here, 1, 0), zs, half_rows], kv_rs.at[zs])
            else:
                received(both, kv_rs.at[zs])
            if not top:
                for role in range(2):
                    go(kv_pass(zs, role), ("pass",), rows)

        def need_kv(zs):
            both = kvb.at[:, zs, other_rows]
            if top:
                @pl.when(c == 1)
                def _():
                    received(both, kp_rs.at[zs])
            else:
                received(both, kp_rs.at[zs])

        def finish_q():
            qb[0] = (acc[WQ] * (HD ** -0.5)).astype(jnp.bfloat16)

        def attend(state, qi, zs):
            qpos = (dp + 2 * qi) * rows + lax.broadcasted_iota(jnp.int32, (rows, 1), 0)
            first = jnp.zeros((rows, 1), jnp.int32)
            for e in ends:
                first = jnp.where(qpos >= e, e, first)
            s = lax.dot_general(
                qb[qi], kvb[0, zs], (((1,), (1,)), ((), ())), preferred_element_type=jnp.float32
            )
            kpos = zs * 2 * rows + lax.broadcasted_iota(jnp.int32, s.shape, 1)
            s = jnp.where((kpos >= first) & (kpos <= qpos), s, jnp.float32(NEG))
            peak = jnp.max(s, axis=1, keepdims=True)
            if state is not None:
                peak = jnp.maximum(state[0], peak)
            p = jnp.exp(s - peak)
            total = jnp.sum(p, axis=1, keepdims=True)
            value = jnp.dot(
                p.astype(jnp.bfloat16), kvb[1, zs], preferred_element_type=jnp.float32
            )
            if state is not None:
                fade = jnp.exp(state[0] - peak)
                total = total + state[1] * fade
                value = value + state[2] * fade
            return peak, total, value

        last = nt - 1

        def go_if(cond, copy, key, rows_sent):
            @pl.when(cond)
            def _():
                copy.start()
            tally(key, rows_sent, cond)

        def wo_arrived(g, ref, h=0):
            received(ref, wi_rs.at[g, h])

        def collect():
            @pl.when(t == z)
            def _():
                for g in range(nt):
                    if g != z:
                        wo_arrived(g, wo_block(g, c))
                    wo_pass(g, c).start()

        def last_hop(way):
            return z == (nz - 2 if way == UP else 1)

        def send_on(g, way, zs):
            if g != loose_block(way):
                for h in range(2):
                    wo_chain(g, way, zs, h).start()
                return
            wo_chain(g, way, zs).start()
            if last_hop(way):
                wo_twin(way, zs).start()

        def hub(way, *picks):
            for k in picks:
                @pl.when(t == z)
                def _():
                    send_on(k if way == UP else (k + 1) % nt, way, z)

        def loose(way):
            size = loose_rows(z, way)
            go_if(
                t == (last if way == UP else 0),
                wo_loose(woc.at[pl.ds(nout - size, size)], z, way), ("x", way), size,
            )

        def relay(way, *picks, only=None, halves=(0, 1)):
            if z == (0 if way == UP else nz - 1):
                return
            ends = z == (nz - 1 if way == UP else 0)
            mine = t < z if way == UP else t > z
            if only is not None:
                mine = t == only
            for k in picks:
                g = k if way == UP else (k + 1) % nt
                if k < nt - 1:
                    @pl.when(mine)
                    def _():
                        for h in halves:
                            wo_arrived(g, wo_piece(g, h), h)
                            if not ends:
                                wo_chain(g, way, None, h).start()
                        if halves[-1] == 1:
                            wo_pass(g, c).start()
                else:
                    for zs in range(z) if way == UP else range(z + 1, nz):
                        @pl.when(t == zs)
                        def _():
                            wo_arrived(g, wo_half(g, 0, zs, way))
                            if not ends:
                                send_on(g, way, zs)

        def relay_loose(way, zs):
            mine = t == (last if way == UP else 0)
            size = loose_rows(zs, way)

            @pl.when(mine)
            def _():
                received(wox.at[zs, pl.ds(0, size)], wx_rs.at[zs])
            if z != (nz - 1 if way == UP else 0):
                go_if(
                    mine, wo_loose(wox.at[zs, pl.ds(0, size)], zs, way), ("x", way), size
                )
            go_if(mine, wo_loose_cross(zs, way), ("cross", way), size)

        def query_copy():
            return remote(qb.at[0], qb.at[1], pt_ss.at[0], pt_rs.at[0], below)

        def part_copies(to):
            return (
                remote(part, pin, pt_ss.at[1], pt_rs.at[1], to),
                remote(lse, lin, pt_ss.at[2], pt_rs.at[2], to),
            )

        order = (KA, KB, WQ) if top else (WQ, KA, KB)
        for item in order:
            loads[item].wait()
            if not top and (bottom or item != KB):
                own_send(item, UP)
            if top or (not bottom and item != WQ):
                own_send(item, DOWN)
            own_send(item, SIDE)
        loads[4].wait()
        go_if(t != z, wo_cross(z), ("own",), nout)

        @pl.when(t == z)
        def _():
            wo_block(t, c)[...] = woc[...]

        loads[3].wait()

        if top:
            @pl.when(c == 0)
            def _():
                kvb[:, z, rows:, :] = jnp.zeros((2, rows, HD), kvb.dtype)

        waiting = [(WQ, z), (KA, z), (KB, z)]

        def step(item, zz, *ways, keep=2):
            event(item, zz, *ways)
            waiting.append((item, zz))
            settle(keep)

        def settle(keep):
            while len(waiting) > keep:
                dot(*waiting.pop(0))

        if bottom:
            step(KA, 1)
            collect()
            loose(UP)
            hub(UP, 0, 1, 2, 3)
            step(KB, 1)
            for zz in range(2, nz):
                step(KA, zz)
                step(KB, zz)
            settle(0)
            finish_kv(KA, KB)
            for zz in range(1, nz):
                step(WQ, zz, keep=1)
            take_kv(z)
            settle(0)
            finish_q()
            need_kv(z)
            state = attend(None, 0, z)
        elif top:
            step(WQ, 2)
            step(KA, 2)
            collect()
            loose(DOWN)
            hub(DOWN, 0, 1, 2, 3)
            step(WQ, 1)
            step(KB, 2)
            step(WQ, 0)
            settle(0)
            finish_q()
            go(query_copy(), ("query",), rows)
            step(KA, 1, keep=1)
            step(KB, 1, keep=1)
            step(KA, 0, keep=1)
            step(KB, 0, keep=1)
            finish_kv(KA)
            settle(0)
            finish_kv(KB)
            take_kv(z)
            need_kv(z)
            peak, total, value = attend(None, 0, z)
            for zz in range(nz - 2, -1, -1):
                relay_loose(UP, zz)
            for copy in part_copies(below):
                copy.wait_recv()
            side = jnp.transpose(jnp.broadcast_to(lin[0:1, :], (HD, rows)))[:, 0:1]
            best = jnp.maximum(peak, side)
            near, far = jnp.exp(peak - best), jnp.exp(side - best)
            state = (
                best, total * near + far, value * near + pin[...].astype(jnp.float32) * far
            )
        elif z == 1:
            step(WQ, 0, UP)
            own_send(KB, UP)
            step(KA, 2, DOWN)
            step(KA, 0, UP)
            step(KB, 2, DOWN)
            step(KA, 3, DOWN)
            step(KB, 0, UP)
            step(KB, 3, DOWN)
            own_send(WQ, DOWN)
            collect()
            settle(0)
            finish_kv(KA, KB)
            loose(UP)
            hub(UP, 0, 1, 2, 3)
            relay(UP, 0, 1, 2, 3)
            relay_loose(UP, 0)
            step(WQ, 2, DOWN)
            step(WQ, 3, DOWN)
            loose(DOWN)
            hub(DOWN, 0, 1, 2, 3)
            take_kv(z)
            settle(0)
            finish_q()
            need_kv(z)
            state = attend(None, 0, z)
            relay(DOWN, 0, 1)
            relay_loose(DOWN, 2)
            relay_loose(DOWN, 3)
            take_kv(0)
            relay(DOWN, 2, 3)
            need_kv(0)
            state = attend(state, 0, 0)
        else:
            step(WQ, 1, UP)
            own_send(KB, UP)
            step(KA, 3, DOWN)
            step(KB, 3, DOWN)
            own_send(WQ, DOWN)
            step(KA, 1)
            step(WQ, 3, DOWN)
            step(WQ, 0, UP)
            go_chain(KA, 1, UP)
            collect()
            loose(DOWN)
            hub(DOWN, 0, 1, 2, 3)
            step(KB, 1, UP)
            relay(DOWN, 0)
            relay_loose(DOWN, 3)
            step(KA, 0, UP)
            relay(DOWN, 1)
            step(KB, 0, UP)
            loose(UP)
            hub(UP, 0)
            settle(0)
            finish_kv(KA, KB)
            finish_q()
            relay(DOWN, 2, 3)
            take_kv(1)
            need_kv(1)
            state = attend(None, 0, 1)
            query_copy().wait_recv()
            other = attend(None, 1, 1)
            take_kv(z)
            need_kv(z)
            other = attend(other, 1, z)
            state = attend(state, 0, z)
            relay(UP, 0, only=1)
            relay_loose(UP, 1)
            relay_loose(UP, 0)
            take_kv(0)
            need_kv(0)
            relay(UP, 0, only=0, halves=(0,))
            peak, total, value = attend(other, 1, 0)
            part[...] = (value / total).astype(jnp.bfloat16)
            lse[...] = jnp.transpose(
                jnp.broadcast_to(peak + jnp.log(total), (rows, HD))
            )[:lse.shape[0], :]
            for copy in part_copies(above):
                copy.start()
            hub(UP, 1, 2, 3)
            relay(UP, 0, only=0, halves=(1,))
            relay(UP, 1, halves=(0,))
            state = attend(state, 0, 0)
            relay(UP, 1, halves=(1,))

        hloc[...] = (state[2] / state[1]).astype(jnp.bfloat16)
        for k in range(1, nt):
            head_copy(k).start()
        head_cols(t)[...] = hloc[...]

        if bottom:
            for zz in range(1, nz):
                relay_loose(DOWN, zz)
            relay(DOWN, 0, 1, 2, 3)
        elif top:
            relay(UP, 0, 1, 2, 3)
        elif z == 2:
            relay(UP, 2, 3)

        for zs in range(nz):
            if zs != z:
                way = UP if zs < z else DOWN
                g = loose_block(way)

                @pl.when(t == zs)
                def _():
                    late = wo_half(g, 1, zs, way)
                    received(late, wx_rs.at[nz])
                    if top or bottom:
                        remote(late, late, wp_ss.at[0], wp_rs.at[0], partner).start()
                    else:
                        wo_pass(g, c).start()
        received(wof.at[pl.ds(pl.multiple_of((1 - c) * nout, 64), nout)], wp_rs.at[0])
        received(hid.at[:, pl.ds(0, (nt - 1) * HD)], h_rs.at[0])
        out_ref[...] = lax.dot_general(
            hcat[...], wof[...], (((1,), (1,)), ((), ())), preferred_element_type=jnp.float32
        ).astype(out_ref.dtype)
        drain(h_ss.at[0], (nt - 1) * rows)
        drain(wp_ss.at[0], (nt - 1) * nout)
        for zs in range(nz):
            way = UP if zs < z else DOWN
            part_only = zs != z and (top or bottom)

            @pl.when(t == zs)
            def _():
                drain(wp_ss.at[0], loose_rows(zs, way) if part_only else nout)
        end_kv()
        if z == nz - 2:
            for copy in part_copies(above):
                copy.wait_send()
        for way, ends_here, mine in ((UP, top, t <= z), (DOWN, bottom, t >= z)):
            if not ends_here:
                @pl.when(mine)
                def _():
                    drain(wc_ss.at[1, way], (nt - 1) * nout)
                for zs in range(z + 1) if way == UP else range(z, nz):
                    @pl.when(t == zs)
                    def _():
                        rest = nout - loose_rows(zs, way)
                        drain(wc_ss.at[0, way], rest * (2 if last_hop(way) else 1))
        for key, (amount, cond) in counts.items():
            sem = {
                "w": lambda: ss.at[key[1], key[2]], "far": lambda: kv_ss.at[0],
                "pass": lambda: kp_ss.at[0], "x": lambda: wx_ss.at[key[1]],
                "cross": lambda: wi_ss.at[1], "own": lambda: wi_ss.at[0],
                "query": lambda: pt_ss.at[0],
            }[key[0]]()
            if cond is None:
                drain(sem, amount)
            else:
                @pl.when(cond)
                def _():
                    drain(sem, amount)

    for z in range(nz):
        @pl.when(plane_of == z)
        def _():
            plane(z)


def fused_body(nz, nt, hidden_states, resp_lengths, w_query, w_keyval, w_out):
    rows, depth = hidden_states.shape
    nout = w_out.shape[1]
    bf16, f32 = jnp.bfloat16, jnp.float32
    dma = pltpu.SemaphoreType.DMA
    hbm = pl.BlockSpec(memory_space=pltpu.HBM)
    return pl.pallas_call(
        functools.partial(fused_kernel, nz, nt),
        out_shape=jax.ShapeDtypeStruct((rows, 2 * nout), bf16),
        in_specs=[hbm] * 5,
        out_specs=pl.BlockSpec(memory_space=pltpu.VMEM),
        scratch_shapes=[
            pltpu.VMEM((rows, depth), bf16),
            pltpu.VMEM((3, depth, HD), bf16),
            pltpu.VMEM((nout, HD), bf16),
            pltpu.VMEM((nz, nout, HD), bf16),
            pltpu.VMEM((2 * nout, nt * HD), bf16),
            pltpu.VMEM((2, rows, HD), bf16),
            pltpu.VMEM((2, nz, 2 * rows, HD), bf16),
            pltpu.VMEM((3, rows, HD), f32),
            pltpu.VMEM((2, rows, HD), bf16),
            pltpu.VMEM((rows, HD), bf16),
            pltpu.VMEM((8, rows), f32),
            pltpu.VMEM((rows, HD), bf16),
            pltpu.VMEM((8, rows), f32),
            pltpu.VMEM((rows, HD), bf16),
            pltpu.VMEM((rows, nt * HD), bf16),
            dma((6,)),
            dma((2, 3)),
            dma((3, nz)),
            dma((3, nz)),
            dma((2,)),
            dma((nz,)),
            dma((1,)),
            dma((nz,)),
            dma((2, 2)),
            dma((2,)),
            dma((nz + 1,)),
            dma((2,)),
            dma((nt, 2)),
            dma((1,)),
            dma((1,)),
            dma((3,)),
            dma((3,)),
            dma((1,)),
            dma((1,)),
            pltpu.SMEM(resp_lengths.shape, jnp.int32),
        ],
        compiler_params=pltpu.CompilerParams(
            collective_id=0, has_side_effects=True, vmem_limit_bytes=40_000_000
        ),
    )(*[
        pltpu.with_memory_space_constraint(x, pltpu.HBM)
        for x in (resp_lengths, hidden_states, w_query, w_keyval, w_out.T)
    ])


def per_device(mesh, hidden_states, resp_lengths, w_query, w_keyval, w_out):
    nt = mesh.shape["tp"]
    nz = mesh.shape["dp"] // 2
    args = (hidden_states, resp_lengths, w_query, w_keyval, w_out)
    fits = (
        mesh.shape["dp"] == 2 * nz and nz == nt and nt == 4
        and w_query.shape[1] == HD and w_keyval.shape[1] == 2 * HD
        and w_out.shape[0] == HD and w_query.shape[0] % 64 == 0
    )
    return fused_body(nz, nt, *args) if fits else body(*args)


def solution(mesh):
    return jax.shard_map(
        functools.partial(per_device, mesh),
        mesh=mesh,
        in_specs=(P("dp", None), P(), P("dp", "tp"), P("dp", "tp"), P("tp", "dp")),
        out_specs=P("dp", "tp"),
        check_vma=False,
    )
```

```python
import functools

import jax
import jax.numpy as jnp
from jax import lax
from jax.experimental import pallas as pl
from jax.experimental.pallas import tpu as pltpu
from jax.sharding import PartitionSpec as P

HD = 128


def segment_of(position, resp_ends):
    return jnp.sum(
        (position[:, None] >= resp_ends[None, :]).astype(jnp.int32), axis=1, dtype=jnp.int32
    )


def body(hidden_states, resp_lengths, w_query, w_keyval, w_out):
    token_rows = hidden_states.shape[0]
    head_scale = HD ** (-0.5)
    pieces = (
        lax.all_gather(w_query, "dp", axis=0, tiled=True),
        lax.all_gather(w_keyval, "dp", axis=0, tiled=True),
    )
    query_sum = jnp.dot(hidden_states, pieces[0], preferred_element_type=jnp.float32)
    keyval_sum = jnp.dot(hidden_states, pieces[1], preferred_element_type=jnp.float32)
    query = (query_sum * head_scale).astype(jnp.bfloat16)
    keyval = lax.all_gather(keyval_sum.astype(jnp.bfloat16), "tp", axis=1, tiled=True)
    kv_count = keyval.shape[1] // (2 * HD)
    per_group = lax.axis_size("tp") // kv_count
    kv_head = lax.axis_index("tp") // per_group
    key_head = lax.dynamic_slice_in_dim(keyval, kv_head * HD, HD, 1)
    value_head = lax.dynamic_slice_in_dim(keyval, (kv_count + kv_head) * HD, HD, 1)
    head_pair = jnp.concatenate([key_head, value_head], axis=1)
    resp_ends = jnp.cumsum(resp_lengths, dtype=jnp.int32)
    own_begin = lax.axis_index("dp") * token_rows
    query_pos = own_begin + jnp.arange(token_rows, dtype=jnp.int32)
    query_seg = segment_of(query_pos, resp_ends)
    pieces = lax.all_gather(head_pair, "dp", axis=0, tiled=True)
    largest = jnp.full((token_rows,), -1e30, jnp.float32)
    height = pieces.shape[0]
    key_pos = jnp.arange(height, dtype=jnp.int32)
    key_seg = segment_of(key_pos, resp_ends)
    scores = jnp.dot(query, pieces[:, :HD].T, preferred_element_type=jnp.float32)
    allowed = (
        (query_seg[:, None] == key_seg[None, :])
        & (key_pos[None, :] <= query_pos[:, None])
        & (key_pos[None, :] >= 0)
    )
    newest = jnp.maximum(largest, jnp.max(jnp.where(allowed, scores, jnp.float32(-1e30)), axis=1))
    expw = jnp.where(allowed, jnp.exp(scores - newest[:, None]), jnp.float32(0.0))
    denom = jnp.sum(expw, axis=1)
    numer = jnp.dot(expw.astype(jnp.bfloat16), pieces[:, HD:], preferred_element_type=jnp.float32)
    heads_out = (numer / denom[:, None]).astype(jnp.bfloat16)
    terms = jnp.dot(
        heads_out,
        lax.all_gather(w_out, "dp", axis=1, tiled=True),
        preferred_element_type=jnp.float32,
    )
    summed = lax.psum_scatter(terms.astype(jnp.bfloat16), "tp", scatter_dimension=1, tiled=True)
    return summed


MESH = pl.DeviceIdType.MESH
KA, KB, WQ = range(3)
UP, DOWN, SIDE = range(3)
NEG = -1e30
LOOSE = ((28, 28, 12, 0), (0, 12, 24, 18))


def fused_kernel(
    nz, nt, lens_hbm, hid_hbm, wq_hbm, wkv_hbm, wo_hbm, out_ref,
    hid, w, woc, wox, wof, kvloc, kvb, acc, qb, part, lse, pin, lin, hloc, hcat,
    loc_sem, ss, rs, prs, kv_ss, kv_rs, kp_ss, kp_rs, wc_ss, wx_ss, wx_rs, wi_ss, wi_rs, wp_ss, wp_rs,
    pt_ss, pt_rs, h_ss, h_rs, lens_ref,
):
    dp = lax.axis_index("dp")
    t = lax.axis_index("tp")
    plane_of, c = dp // 2, dp % 2
    rows = hid.shape[0]
    shard = wq_hbm.shape[0]
    nout = wo_hbm.shape[0]
    own = pl.ds(pl.multiple_of(dp * shard, 64), shard)

    barrier = pltpu.get_barrier_semaphore()
    partner = {"dp": dp + 1 - 2 * c, "tp": t}
    above, below = {"dp": dp + 2, "tp": t}, {"dp": dp - 2, "tp": t}
    has_up, has_down = plane_of < nz - 1, plane_of > 0
    pl.semaphore_signal(barrier, 1, device_id=partner, device_id_type=MESH)

    @pl.when(has_up)
    def _():
        pl.semaphore_signal(barrier, 1, device_id=above, device_id_type=MESH)

    @pl.when(has_down)
    def _():
        pl.semaphore_signal(barrier, 1, device_id=below, device_id_type=MESH)

    for k in range(1, nt):
        pl.semaphore_signal(
            barrier, 1, device_id={"dp": dp, "tp": (t + k) % nt}, device_id_type=MESH
        )
    loads = [
        pltpu.make_async_copy(wkv_hbm.at[:, pl.ds(0, HD)], w.at[KA, own], loc_sem.at[KA]),
        pltpu.make_async_copy(wkv_hbm.at[:, pl.ds(HD, HD)], w.at[KB, own], loc_sem.at[KB]),
        pltpu.make_async_copy(wq_hbm, w.at[WQ, own], loc_sem.at[WQ]),
        pltpu.make_async_copy(hid_hbm, hid, loc_sem.at[3]),
        pltpu.make_async_copy(wo_hbm, woc, loc_sem.at[4]),
        pltpu.make_async_copy(lens_hbm, lens_ref, loc_sem.at[5]),
    ]
    for load in loads:
        load.start()

    pl.semaphore_wait(barrier, nt + has_up.astype(jnp.int32) + has_down.astype(jnp.int32))

    def chunk(item, zz, cc):
        return w.at[item, pl.ds(pl.multiple_of((2 * zz + cc) * shard, 64), shard)]

    def remote(src, dst, send, recv, to):
        return pltpu.make_async_remote_copy(
            src, dst, send, recv, device_id=to, device_id_type=MESH
        )

    def chain(item, zz, way):
        ref = chunk(item, zz, c)
        recv = prs.at[item, zz] if way == SIDE else rs.at[item, zz]
        return remote(
            ref, ref, ss.at[int(item == WQ), way], recv, (above, below, partner)[way]
        )

    def device(zz, tt):
        return {"dp": 2 * zz + c, "tp": tt}

    half_rows = pl.ds(pl.multiple_of(c * rows, 128), rows)
    other_rows = pl.ds(pl.multiple_of((1 - c) * rows, 128), rows)

    def kv_copy(z, b, zz):
        role = t // (nt // 2)
        return remote(
            kvloc.at[b], kvb.at[role, z, half_rows], kv_ss.at[int(zz == z)], kv_rs.at[z],
            device(zz, 2 * (t % (nt // 2)) + b),
        )

    def kv_over(z, b):
        role = t // (nt // 2)
        return remote(
            kvloc.at[b], kvb.at[role, z, pl.ds(0, rows)], kp_ss.at[0], kp_rs.at[z],
            {"dp": dp + 1, "tp": 2 * (t % (nt // 2)) + b},
        )

    def kv_pass(z, role):
        ref = kvb.at[role, z, half_rows]
        return remote(ref, ref, kp_ss.at[0], kp_rs.at[z], partner)

    def wo_block(g, cc):
        return wof.at[
            pl.ds(pl.multiple_of(cc * nout, 64), nout), pl.ds(pl.multiple_of(g * HD, HD), HD)
        ]

    def loose_rows(zs, way):
        return nout * LOOSE[way][zs] // 512 * 16

    def wo_half(g, h, zs, way):
        split = nout - loose_rows(zs, way)
        start = pl.multiple_of(c * nout + h * split, 16)
        size = nout - split if h else split
        return wof.at[pl.ds(start, size), pl.ds(pl.multiple_of(g * HD, HD), HD)]

    def loose_block(way):
        return nt - 1 if way == UP else 0

    def wo_piece(g, h):
        start = pl.multiple_of(c * nout + h * (nout // 2), 16)
        return wof.at[pl.ds(start, nout // 2), pl.ds(pl.multiple_of(g * HD, HD), HD)]

    def wo_chain(g, way, zs, h=0):
        full = int(g != loose_block(way))
        ref = wo_piece(g, h) if full else wo_half(g, 0, zs, way)
        return remote(ref, ref, wc_ss.at[full, way], wi_rs.at[g, h], (above, below)[way])

    def wo_twin(way, zs):
        ref = wo_half(loose_block(way), 0, zs, way)
        to = {"dp": dp + (2 if way == UP else -2) + 1 - 2 * c, "tp": t}
        return remote(ref, ref, wc_ss.at[0, way], wp_rs.at[0], to)

    def wo_loose(src, zz, way):
        return remote(
            src, wox.at[zz, pl.ds(0, loose_rows(zz, way))], wx_ss.at[way], wx_rs.at[zz],
            (above, below)[way],
        )

    def wo_cross(zz):
        return remote(woc, wo_block(t, c), wi_ss.at[0], wi_rs.at[t, 0], {"dp": dp, "tp": zz})

    def wo_loose_cross(zz, way):
        return remote(
            wox.at[zz, pl.ds(0, loose_rows(zz, way))], wo_half(t, 1, zz, way), wi_ss.at[1],
            wx_rs.at[nz], {"dp": dp, "tp": zz},
        )

    def wo_pass(g, cc):
        ref = wo_block(g, cc)
        return remote(ref, ref, wp_ss.at[0], wp_rs.at[0], partner)

    def head_cols(g):
        return hcat.at[:, pl.ds(pl.multiple_of(g * HD, HD), HD)]

    def head_copy(k):
        return remote(
            hloc, head_cols(t), h_ss.at[0], h_rs.at[0], {"dp": dp, "tp": (t + k) % nt}
        )

    loads[5].wait()
    ends = []
    end = jnp.int32(0)
    for r in range(lens_ref.shape[0]):
        end = end + lens_ref[r]
        ends.append(end)

    def plane(z):
        counts = {}
        seen = set()
        top, bottom = z == nz - 1, z == 0
        kv_to = [zz for zz in (nz - 2, nz - 3, 0) if zz >= z] if not top else [z]
        span = 2 * shard

        def tally(key, rows_sent, cond=None):
            counts[key] = (counts.get(key, (0, cond))[0] + rows_sent, cond)

        def go(copy, key, rows_sent):
            copy.start()
            tally(key, rows_sent)

        def go_chain(item, zz, way):
            go(chain(item, zz, way), ("w", int(item == WQ), way), shard)

        def received(ref, sem):
            remote(ref, ref, sem, sem, partner).wait_recv()

        def drain(sem, amount):
            ref = w.at[0, pl.ds(0, amount)]
            remote(ref, ref, sem, sem, partner).wait_send()

        def own_send(item, way):
            go_chain(item, z, way)

        def event(item, zz, *ways):
            ref = chunk(item, zz, c)
            received(ref, rs.at[item, zz])
            for way in ways + (SIDE,):
                go_chain(item, zz, way)

        def dot(item, zz):
            ref = chunk(item, zz, 1 - c)
            received(ref, prs.at[item, zz])
            part_sum = jnp.dot(
                hid[:, zz * span:(zz + 1) * span], w[item, zz * span:(zz + 1) * span, :],
                preferred_element_type=jnp.float32,
            )
            if item in seen:
                acc[item] += part_sum
            else:
                seen.add(item)
                acc[item] = part_sum

        def finish_kv(*picks):
            role = t // (nt // 2)
            for b in picks:
                kvloc[b] = acc[b].astype(jnp.bfloat16)
            for zz in kv_to:
                if zz != z:
                    for b in picks:
                        go(kv_copy(z, b, zz), ("far",), rows)
            for b in picks:
                mine = 2 * (t % (nt // 2)) + b == t
                if top:
                    go_if(c == 0, kv_over(z, b), ("pass",), rows)

                @pl.when(jnp.logical_not(mine))
                def _():
                    kv_copy(z, b, z).start()

                @pl.when(mine)
                def _():
                    kvb[role, z, half_rows, :] = kvloc[b]

        k_here, v_here = t // 2 == t, t // 2 + nt // 2 == t
        none_here = jnp.logical_not(jnp.logical_or(k_here, v_here))

        def end_kv():
            @pl.when(none_here)
            def _():
                drain(kv_ss.at[1], 2 * rows)

            @pl.when(jnp.logical_not(none_here))
            def _():
                drain(kv_ss.at[1], rows)

        def take_kv(zs):
            both = kvb.at[:, zs, half_rows]
            if zs == z:
                @pl.when(none_here)
                def _():
                    received(both, kv_rs.at[zs])

                @pl.when(jnp.logical_not(none_here))
                def _():
                    received(kvb.at[jnp.where(k_here, 1, 0), zs, half_rows], kv_rs.at[zs])
            else:
                received(both, kv_rs.at[zs])
            if not top:
                for role in range(2):
                    go(kv_pass(zs, role), ("pass",), rows)

        def need_kv(zs):
            both = kvb.at[:, zs, other_rows]
            if top:
                @pl.when(c == 1)
                def _():
                    received(both, kp_rs.at[zs])
            else:
                received(both, kp_rs.at[zs])

        def finish_q():
            qb[0] = (acc[WQ] * (HD ** -0.5)).astype(jnp.bfloat16)

        def attend(state, qi, zs):
            qpos = (dp + 2 * qi) * rows + lax.broadcasted_iota(jnp.int32, (rows, 1), 0)
            first = jnp.zeros((rows, 1), jnp.int32)
            for e in ends:
                first = jnp.where(qpos >= e, e, first)
            s = lax.dot_general(
                qb[qi], kvb[0, zs], (((1,), (1,)), ((), ())), preferred_element_type=jnp.float32
            )
            kpos = zs * 2 * rows + lax.broadcasted_iota(jnp.int32, s.shape, 1)
            s = jnp.where((kpos >= first) & (kpos <= qpos), s, jnp.float32(NEG))
            peak = jnp.max(s, axis=1, keepdims=True)
            if state is not None:
                peak = jnp.maximum(state[0], peak)
            p = jnp.exp(s - peak)
            total = jnp.sum(p, axis=1, keepdims=True)
            value = jnp.dot(
                p.astype(jnp.bfloat16), kvb[1, zs], preferred_element_type=jnp.float32
            )
            if state is not None:
                fade = jnp.exp(state[0] - peak)
                total = total + state[1] * fade
                value = value + state[2] * fade
            return peak, total, value

        last = nt - 1

        def go_if(cond, copy, key, rows_sent):
            @pl.when(cond)
            def _():
                copy.start()
            tally(key, rows_sent, cond)

        def wo_arrived(g, ref, h=0):
            received(ref, wi_rs.at[g, h])

        def collect():
            @pl.when(t == z)
            def _():
                for g in range(nt):
                    if g != z:
                        wo_arrived(g, wo_block(g, c))
                    wo_pass(g, c).start()

        def last_hop(way):
            return z == (nz - 2 if way == UP else 1)

        def send_on(g, way, zs):
            if g != loose_block(way):
                for h in range(2):
                    wo_chain(g, way, zs, h).start()
                return
            wo_chain(g, way, zs).start()
            if last_hop(way):
                wo_twin(way, zs).start()

        def hub(way, *picks):
            for k in picks:
                @pl.when(t == z)
                def _():
                    send_on(k if way == UP else (k + 1) % nt, way, z)

        def loose(way):
            size = loose_rows(z, way)
            go_if(
                t == (last if way == UP else 0),
                wo_loose(woc.at[pl.ds(nout - size, size)], z, way), ("x", way), size,
            )

        def relay(way, *picks, only=None, halves=(0, 1)):
            if z == (0 if way == UP else nz - 1):
                return
            ends = z == (nz - 1 if way == UP else 0)
            mine = t < z if way == UP else t > z
            if only is not None:
                mine = t == only
            for k in picks:
                g = k if way == UP else (k + 1) % nt
                if k < nt - 1:
                    @pl.when(mine)
                    def _():
                        for h in halves:
                            wo_arrived(g, wo_piece(g, h), h)
                            if not ends:
                                wo_chain(g, way, None, h).start()
                        if halves[-1] == 1:
                            wo_pass(g, c).start()
                else:
                    for zs in range(z) if way == UP else range(z + 1, nz):
                        @pl.when(t == zs)
                        def _():
                            wo_arrived(g, wo_half(g, 0, zs, way))
                            if not ends:
                                send_on(g, way, zs)

        def relay_loose(way, zs):
            mine = t == (last if way == UP else 0)
            size = loose_rows(zs, way)

            @pl.when(mine)
            def _():
                received(wox.at[zs, pl.ds(0, size)], wx_rs.at[zs])
            if z != (nz - 1 if way == UP else 0):
                go_if(
                    mine, wo_loose(wox.at[zs, pl.ds(0, size)], zs, way), ("x", way), size
                )
            go_if(mine, wo_loose_cross(zs, way), ("cross", way), size)

        def query_copy():
            return remote(qb.at[0], qb.at[1], pt_ss.at[0], pt_rs.at[0], below)

        def part_copies(to):
            return (
                remote(part, pin, pt_ss.at[1], pt_rs.at[1], to),
                remote(lse, lin, pt_ss.at[2], pt_rs.at[2], to),
            )

        order = (KA, KB, WQ) if top else (WQ, KA, KB)
        for item in order:
            loads[item].wait()
            if not top and (bottom or item != KB):
                own_send(item, UP)
            if top or (not bottom and item != WQ):
                own_send(item, DOWN)
            own_send(item, SIDE)
        loads[4].wait()
        go_if(t != z, wo_cross(z), ("own",), nout)

        @pl.when(t == z)
        def _():
            wo_block(t, c)[...] = woc[...]

        loads[3].wait()

        if top:
            @pl.when(c == 0)
            def _():
                kvb[:, z, rows:, :] = jnp.zeros((2, rows, HD), kvb.dtype)

        waiting = [(WQ, z), (KA, z), (KB, z)]

        def step(item, zz, *ways, keep=2):
            event(item, zz, *ways)
            waiting.append((item, zz))
            settle(keep)

        def settle(keep):
            while len(waiting) > keep:
                dot(*waiting.pop(0))

        if bottom:
            step(KA, 1)
            collect()
            loose(UP)
            hub(UP, 0, 1, 2, 3)
            step(KB, 1)
            for zz in range(2, nz):
                step(KA, zz)
                step(KB, zz)
            settle(0)
            finish_kv(KA, KB)
            for zz in range(1, nz):
                step(WQ, zz, keep=1)
            take_kv(z)
            settle(0)
            finish_q()
            need_kv(z)
            state = attend(None, 0, z)
        elif top:
            step(WQ, 2)
            step(KA, 2)
            collect()
            loose(DOWN)
            hub(DOWN, 0, 1, 2, 3)
            step(WQ, 1)
            step(KB, 2)
            step(WQ, 0)
            settle(0)
            finish_q()
            go(query_copy(), ("query",), rows)
            step(KA, 1, keep=1)
            step(KB, 1, keep=1)
            step(KA, 0, keep=1)
            step(KB, 0, keep=1)
            finish_kv(KA)
            settle(0)
            finish_kv(KB)
            take_kv(z)
            need_kv(z)
            peak, total, value = attend(None, 0, z)
            for zz in range(nz - 2, -1, -1):
                relay_loose(UP, zz)
            for copy in part_copies(below):
                copy.wait_recv()
            side = jnp.transpose(jnp.broadcast_to(lin[0:1, :], (HD, rows)))[:, 0:1]
            best = jnp.maximum(peak, side)
            near, far = jnp.exp(peak - best), jnp.exp(side - best)
            state = (
                best, total * near + far, value * near + pin[...].astype(jnp.float32) * far
            )
        elif z == 1:
            step(WQ, 0, UP)
            own_send(KB, UP)
            step(KA, 2, DOWN)
            step(KA, 0, UP)
            step(KB, 2, DOWN)
            step(KA, 3, DOWN)
            step(KB, 0, UP)
            step(KB, 3, DOWN)
            own_send(WQ, DOWN)
            collect()
            settle(0)
            finish_kv(KA, KB)
            loose(UP)
            hub(UP, 0, 1, 2, 3)
            relay(UP, 0, 1, 2, 3)
            relay_loose(UP, 0)
            step(WQ, 2, DOWN)
            step(WQ, 3, DOWN)
            loose(DOWN)
            hub(DOWN, 0, 1, 2, 3)
            take_kv(z)
            settle(0)
            finish_q()
            need_kv(z)
            state = attend(None, 0, z)
            relay(DOWN, 0, 1)
            relay_loose(DOWN, 2)
            relay_loose(DOWN, 3)
            take_kv(0)
            relay(DOWN, 2, 3)
            need_kv(0)
            state = attend(state, 0, 0)
        else:
            step(WQ, 1, UP)
            own_send(KB, UP)
            step(KA, 3, DOWN)
            step(KB, 3, DOWN)
            own_send(WQ, DOWN)
            step(KA, 1)
            step(WQ, 3, DOWN)
            step(WQ, 0, UP)
            go_chain(KA, 1, UP)
            collect()
            loose(DOWN)
            hub(DOWN, 0, 1, 2, 3)
            step(KB, 1, UP)
            relay(DOWN, 0)
            relay_loose(DOWN, 3)
            step(KA, 0, UP)
            relay(DOWN, 1)
            step(KB, 0, UP)
            loose(UP)
            hub(UP, 0)
            settle(0)
            finish_kv(KA, KB)
            finish_q()
            relay(DOWN, 2, 3)
            take_kv(1)
            need_kv(1)
            state = attend(None, 0, 1)
            query_copy().wait_recv()
            other = attend(None, 1, 1)
            take_kv(z)
            need_kv(z)
            other = attend(other, 1, z)
            state = attend(state, 0, z)
            relay(UP, 0, only=1)
            relay_loose(UP, 1)
            relay_loose(UP, 0)
            take_kv(0)
            need_kv(0)
            relay(UP, 0, only=0, halves=(0,))
            peak, total, value = attend(other, 1, 0)
            part[...] = (value / total).astype(jnp.bfloat16)
            lse[...] = jnp.transpose(
                jnp.broadcast_to(peak + jnp.log(total), (rows, HD))
            )[:lse.shape[0], :]
            for copy in part_copies(above):
                copy.start()
            hub(UP, 1, 2, 3)
            relay(UP, 0, only=0, halves=(1,))
            relay(UP, 1)
            state = attend(state, 0, 0)

        hloc[...] = (state[2] / state[1]).astype(jnp.bfloat16)
        for k in range(1, nt):
            head_copy(k).start()
        head_cols(t)[...] = hloc[...]

        if bottom:
            for zz in range(1, nz):
                relay_loose(DOWN, zz)
            relay(DOWN, 0, 1, 2, 3)
        elif top:
            relay(UP, 0, 1, 2, 3)
        elif z == 2:
            relay(UP, 2, 3)

        for zs in range(nz):
            if zs != z:
                way = UP if zs < z else DOWN
                g = loose_block(way)

                @pl.when(t == zs)
                def _():
                    late = wo_half(g, 1, zs, way)
                    received(late, wx_rs.at[nz])
                    if top or bottom:
                        remote(late, late, wp_ss.at[0], wp_rs.at[0], partner).start()
                    else:
                        wo_pass(g, c).start()
        received(wof.at[pl.ds(pl.multiple_of((1 - c) * nout, 64), nout)], wp_rs.at[0])
        received(hid.at[:, pl.ds(0, (nt - 1) * HD)], h_rs.at[0])
        out_ref[...] = lax.dot_general(
            hcat[...], wof[...], (((1,), (1,)), ((), ())), preferred_element_type=jnp.float32
        ).astype(out_ref.dtype)
        drain(h_ss.at[0], (nt - 1) * rows)
        drain(wp_ss.at[0], (nt - 1) * nout)
        for zs in range(nz):
            way = UP if zs < z else DOWN
            part_only = zs != z and (top or bottom)

            @pl.when(t == zs)
            def _():
                drain(wp_ss.at[0], loose_rows(zs, way) if part_only else nout)
        end_kv()
        if z == nz - 2:
            for copy in part_copies(above):
                copy.wait_send()
        for way, ends_here, mine in ((UP, top, t <= z), (DOWN, bottom, t >= z)):
            if not ends_here:
                @pl.when(mine)
                def _():
                    drain(wc_ss.at[1, way], (nt - 1) * nout)
                for zs in range(z + 1) if way == UP else range(z, nz):
                    @pl.when(t == zs)
                    def _():
                        rest = nout - loose_rows(zs, way)
                        drain(wc_ss.at[0, way], rest * (2 if last_hop(way) else 1))
        for key, (amount, cond) in counts.items():
            sem = {
                "w": lambda: ss.at[key[1], key[2]], "far": lambda: kv_ss.at[0],
                "pass": lambda: kp_ss.at[0], "x": lambda: wx_ss.at[key[1]],
                "cross": lambda: wi_ss.at[1], "own": lambda: wi_ss.at[0],
                "query": lambda: pt_ss.at[0],
            }[key[0]]()
            if cond is None:
                drain(sem, amount)
            else:
                @pl.when(cond)
                def _():
                    drain(sem, amount)

    for z in range(nz):
        @pl.when(plane_of == z)
        def _():
            plane(z)


def fused_body(nz, nt, hidden_states, resp_lengths, w_query, w_keyval, w_out):
    rows, depth = hidden_states.shape
    nout = w_out.shape[1]
    bf16, f32 = jnp.bfloat16, jnp.float32
    dma = pltpu.SemaphoreType.DMA
    hbm = pl.BlockSpec(memory_space=pltpu.HBM)
    return pl.pallas_call(
        functools.partial(fused_kernel, nz, nt),
        out_shape=jax.ShapeDtypeStruct((rows, 2 * nout), bf16),
        in_specs=[hbm] * 5,
        out_specs=pl.BlockSpec(memory_space=pltpu.VMEM),
        scratch_shapes=[
            pltpu.VMEM((rows, depth), bf16),
            pltpu.VMEM((3, depth, HD), bf16),
            pltpu.VMEM((nout, HD), bf16),
            pltpu.VMEM((nz, nout, HD), bf16),
            pltpu.VMEM((2 * nout, nt * HD), bf16),
            pltpu.VMEM((2, rows, HD), bf16),
            pltpu.VMEM((2, nz, 2 * rows, HD), bf16),
            pltpu.VMEM((3, rows, HD), f32),
            pltpu.VMEM((2, rows, HD), bf16),
            pltpu.VMEM((rows, HD), bf16),
            pltpu.VMEM((8, rows), f32),
            pltpu.VMEM((rows, HD), bf16),
            pltpu.VMEM((8, rows), f32),
            pltpu.VMEM((rows, HD), bf16),
            pltpu.VMEM((rows, nt * HD), bf16),
            dma((6,)),
            dma((2, 3)),
            dma((3, nz)),
            dma((3, nz)),
            dma((2,)),
            dma((nz,)),
            dma((1,)),
            dma((nz,)),
            dma((2, 2)),
            dma((2,)),
            dma((nz + 1,)),
            dma((2,)),
            dma((nt, 2)),
            dma((1,)),
            dma((1,)),
            dma((3,)),
            dma((3,)),
            dma((1,)),
            dma((1,)),
            pltpu.SMEM(resp_lengths.shape, jnp.int32),
        ],
        compiler_params=pltpu.CompilerParams(
            collective_id=0, has_side_effects=True, vmem_limit_bytes=40_000_000
        ),
    )(*[
        pltpu.with_memory_space_constraint(x, pltpu.HBM)
        for x in (resp_lengths, hidden_states, w_query, w_keyval, w_out.T)
    ])


def per_device(mesh, hidden_states, resp_lengths, w_query, w_keyval, w_out):
    nt = mesh.shape["tp"]
    nz = mesh.shape["dp"] // 2
    args = (hidden_states, resp_lengths, w_query, w_keyval, w_out)
    fits = (
        mesh.shape["dp"] == 2 * nz and nz == nt and nt == 4
        and w_query.shape[1] == HD and w_keyval.shape[1] == 2 * HD
        and w_out.shape[0] == HD and w_query.shape[0] % 64 == 0
    )
    return fused_body(nz, nt, *args) if fits else body(*args)


def solution(mesh):
    return jax.shard_map(
        functools.partial(per_device, mesh),
        mesh=mesh,
        in_specs=(P("dp", None), P(), P("dp", "tp"), P("dp", "tp"), P("tp", "dp")),
        out_specs=P("dp", "tp"),
        check_vma=False,
    )
```
